128 devices in a mesh: aux: 8 (over z_hi, y), pair: 16 (over z_lo, x, core).
Axes of the slice: x: 4, y: 4, z: 4 (z_hi: 2, z_lo: 2; z = z_hi * 2 + z_lo), core: 2. Of those that a mesh axis runs over, the one named last changes fastest.
Arguments:
- m_panels: bfloat16 [40000, 16384], P('aux', 'pair'), may hold values from -6 to 6
- lower_cols: bfloat16 [2, 512, 40000], P(None, 'pair', 'aux'), may hold values from -0.2 to 0.2, as said below
- diag_inverses: float32 [2, 512, 512], replicated, may hold values from -0.2 to 2, as said below
Outputs:
- remainder: bfloat16 [40000, 16384], P('aux', 'pair')
- solved: bfloat16 [2, 512, 16384], P(None, None, 'pair')
The draws below stay inside these ranges and needn't reach their ends.
Inputs may be any that keep to these rules, and one draw needn't show every extreme that they name: lower_cols[k] is zero in the pivot rows of panels 0 to k (the factor is lower triangular and its diagonal blocks are given by their inverses). Each diag_inverses[k] is lower triangular.
All inputs are finite; a program needn't handle non-finite values.
Results may differ from the reference program's by a relative error of at most 0.0047.
Values may be sent and summed in bfloat16 or wider, within the bound.
A program may use at most 192 MiB of HBM per device.

```python
import jax
import jax.numpy as jnp
from jax import lax

NAUX = 40000
NB = 512
PANELS = 2
PAIR_DEV = 1024
AUX_ROWS = 5000
NPAIR = 16384
N_PAIR = 16


def draw_lower_cols(key, part):
    scale = 1.0 / (PANELS * NB) ** 0.5
    values = jnp.clip(jax.random.normal(key, (PANELS, NB, NAUX), jnp.float32), -6.0, 6.0)
    rows = jnp.arange(NAUX, dtype=jnp.int32)
    block = rows // AUX_ROWS
    within = rows % AUX_ROWS
    panel = jnp.arange(PANELS, dtype=jnp.int32)[:, None]
    keep = jnp.logical_not(jnp.logical_and(within[None, :] < NB, block[None, :] <= panel))
    values = jnp.clip(values * scale, -0.199, 0.199) * keep.astype(jnp.float32)[:, None, :]
    return values.astype(jnp.bfloat16)


def draw_diag_inverses(key, part):
    first = jax.random.fold_in(key, 11)
    second = jax.random.fold_in(key, 12)
    lower = jnp.clip(jax.random.normal(first, (PANELS, NB, NB), jnp.float32), -6.0, 6.0)
    lower = jnp.clip(lower * (0.7 / NB ** 0.5), -0.199, 0.199) * jnp.tril(jnp.ones((NB, NB), jnp.float32), -1)[None]
    diagonal = jnp.exp(jax.random.uniform(second, (PANELS, NB), jnp.float32, -0.69, 0.69))
    return lower + diagonal[:, :, None] * jnp.eye(NB, dtype=jnp.float32)[None]


def levels(own_key, extent, split, smallest, high):
    factor_of, own = 1.0, jax.random.fold_in(own_key, 6)
    for dim, parts in split:
        heights = jnp.exp(jax.random.uniform(jax.random.fold_in(own, dim), (parts,), jnp.float32, smallest / len(split), high / len(split)))
        factor_of = factor_of * jnp.repeat(heights, extent[dim] // parts).reshape([-1 if axis == dim else 1 for axis in range(len(extent))])
    return factor_of


def scatter_about(rng, extent, spread, most, split=(), held_as=jnp.bfloat16):
    drawn = spread * jax.random.normal(rng, extent, jnp.float32)
    if split:
        drawn = drawn * levels(rng, extent, split, -0.22, 0.18)
    return jnp.clip(drawn, -most, most).astype(held_as)


def setup_inputs(seed: int = 0) -> dict:
    key_list = jax.random.split(jax.random.key(seed), 4)
    m_panels = scatter_about(key_list[0], (NAUX, NPAIR), 1.0, 6.0, ((0, 8), (1, 16)))
    lower_cols = draw_lower_cols(jax.random.fold_in(key_list[3], 71), 0)
    diag_inverses = draw_diag_inverses(jax.random.fold_in(key_list[3], 71), 0)
    return dict(m_panels=m_panels, lower_cols=lower_cols, diag_inverses=diag_inverses)


def one_group(block_cols, lower_cols, diag_inverses):
    work = block_cols.astype(jnp.float32)
    results = []
    for panel in range(PANELS):
        first = panel * AUX_ROWS
        pivot = work[first:first + NB]
        solved_rows = jnp.dot(diag_inverses[panel], pivot, precision=lax.Precision.HIGHEST, preferred_element_type=jnp.float32).astype(jnp.bfloat16)
        work = work - jnp.dot(lower_cols[panel].T, solved_rows, preferred_element_type=jnp.float32)
        results.append(solved_rows)
    return work.astype(jnp.bfloat16), jnp.stack(results)


def reference(m_panels, lower_cols, diag_inverses):
    groups = m_panels.reshape(NAUX, N_PAIR, PAIR_DEV).transpose(1, 0, 2)
    remains, solves = lax.map(lambda cols: one_group(cols, lower_cols, diag_inverses), groups)
    remainder = remains.transpose(1, 0, 2).reshape(NAUX, N_PAIR * PAIR_DEV)
    solved = solves.transpose(1, 2, 0, 3).reshape(PANELS, NB, N_PAIR * PAIR_DEV)
    return remainder, solved
```

```python
import functools

import jax
import jax.numpy as jnp
from jax import lax
from jax.experimental import pallas as pl
from jax.experimental.pallas import tpu as pltpu
from jax.sharding import PartitionSpec as P

MESH = pl.DeviceIdType.MESH
TYPES = "AABAABAA"
CHUNK = 640
NP = 8
ORDER = (
    (0, (('Py+', 0, 0), ('Py+', 0, 4), ('Py-', 0, 0), ('Py-', 0, 6), ('X', 0, 0), ('X', 0, 1), ('X', 0, 2))),
    (1, (('Py+', 1, 0), ('Py+', 1, 6), ('Py-', 1, 0), ('Py-', 1, 4), ('X', 1, 0), ('X', 1, 1), ('X', 1, 2))),
    ('od', 0),
    ('od', 1),
    ('od', 2),
    ('od', 3),
    ('od', 4),
    ('od', 5),
    ('od', 6),
    ('od', 7),
    ('ou', 0),
    ('ou', 1),
    ('oz', 0),
    ('ou', 2),
    (0, (('X', 0, 3),)),
    (1, (('X', 1, 3),)),
    ('oz', 1),
    (0, (('Py+', 0, 5), ('Py-', 0, 7), ('R', 0, 0))),
    (1, (('Py+', 1, 7), ('Py-', 1, 5), ('R', 1, 0))),
    (4, (('R', 0, 0),)),
    (5, (('R', 1, 0),)),
    ('g', 0),
    ('f', 0),
    ('oz', 2),
    (0, (('R', 0, 1), ('P', 1, 0))),
    (1, (('R', 1, 1), ('P', 0, 0))),
    (3, (('P', 0, 0),)),
    (5, (('R', 1, 1),)),
    ('oz', 'V'),
    (0, (('Py+', 0, 1), ('Py-', 0, 1))),
    (1, (('Py+', 1, 1), ('Py-', 1, 1))),
    (2, (('P', 1, 0),)),
    (4, (('R', 0, 1),)),
    ('f', 1),
    ('g', 1),
    (0, (('R', 0, 2),)),
    (1, (('R', 1, 2),)),
    (4, (('R', 0, 2),)),
    (5, (('R', 1, 2),)),
    ('f', 2),
    ('g', 2),
    (0, (('P', 1, 4),)),
    (1, (('P', 0, 4),)),
    (2, (('P', 1, 6),)),
    (3, (('P', 0, 6),)),
    (4, (('R', 0, 3),)),
    (5, (('R', 1, 3),)),
    ('z', 0),
    (0, (('Py+', 0, 2), ('Py-', 0, 2))),
    (1, (('Py+', 1, 2), ('Py-', 1, 2))),
    (4, (('P', 0, 0),)),
    (5, (('P', 1, 0),)),
    ('oz', 3),
    (0, (('R', 0, 3), ('P', 1, 5))),
    (1, (('R', 1, 3), ('P', 0, 5))),
    (2, (('P', 0, 0), ('P', 1, 7))),
    (3, (('P', 1, 0), ('P', 0, 7))),
    (4, (('P', 0, 1),)),
    (5, (('P', 1, 1),)),
    ('ou', 3),
    (0, (('Py+', 0, 3), ('Py-', 0, 3))),
    (1, (('Py+', 1, 3), ('Py-', 1, 3))),
    (7, (('R', 0, 6),)),
    ('z', 1),
    (2, (('P', 0, 6),)),
    (3, (('P', 1, 6),)),
    (4, (('P', 0, 2),)),
    (5, (('P', 1, 2),)),
    (6, (('R', 1, 6),)),
    ('z', 2),
    ('ou', 4),
    (0, (('P', 1, 1),)),
    (1, (('P', 0, 1),)),
    (2, (('P', 1, 1),)),
    (3, (('P', 0, 1),)),
    (4, (('R', 1, 4),)),
    (5, (('R', 0, 4),)),
    ('z', 'V'),
    (0, (('Py+', 0, 6), ('Py-', 0, 4))),
    (1, (('Py+', 1, 4), ('Py-', 1, 6))),
    (2, (('R', 1, 6),)),
    (4, (('P', 1, 0),)),
    (5, (('P', 0, 0),)),
    (6, (('P', 1, 0), ('R', 1, 7))),
    (7, (('R', 0, 7), ('P', 0, 0))),
    ('oz', 4),
    (3, (('R', 0, 6),)),
    ('g', 3),
    ('zf', 2),
    (2, (('P', 0, 7),)),
    ('ou', 5),
    (0, (('P', 1, 2),)),
    (1, (('P', 0, 2),)),
    (2, (('P', 1, 2),)),
    (3, (('P', 1, 7), ('P', 0, 2))),
    (4, (('R', 1, 5),)),
    (5, (('R', 0, 5),)),
    ('oz', 5),
    ('g', 'V'),
    (0, (('Py+', 0, 7), ('Py-', 0, 5))),
    (1, (('Py+', 1, 5), ('Py-', 1, 7))),
    (4, (('P', 1, 1),)),
    (5, (('P', 0, 1),)),
    (6, (('P', 1, 1),)),
    (7, (('P', 0, 1),)),
    ('f', 3),
    ('zg', 2),
    (3, (('R', 0, 7),)),
    (4, (('P', 0, 3),)),
    (5, (('P', 1, 3),)),
    ('o', 0),
    (2, (('R', 1, 7),)),
    (6, (('P', 1, 6),)),
    (7, (('P', 0, 6),)),
    ('g', 4),
    ('f', 'V'),
    ('zf', 0),
    (0, (('R', 1, 4), ('P', 1, 3))),
    (1, (('R', 0, 4), ('P', 0, 3))),
    (2, (('P', 0, 1), ('P', 1, 3))),
    (3, (('P', 1, 1), ('P', 0, 3))),
    (4, (('P', 1, 2),)),
    (5, (('P', 0, 2),)),
    (6, (('P', 0, 0), ('P', 1, 2))),
    (7, (('P', 1, 0), ('P', 0, 2))),
    ('zf', 1),
    ('o', 1),
    ('z', 3),
    ('f', 4),
    ('f', 5),
    ('zf', 'V'),
    ('oz', 6),
    (0, (('R', 1, 5), ('P', 1, 6))),
    (1, (('R', 0, 5),)),
    (2, (('P', 0, 2), ('P', 1, 4))),
    (3, (('P', 1, 2), ('P', 0, 4))),
    (6, (('P', 1, 7),)),
    (7, (('P', 0, 7),)),
    ('o', 2),
    (1, (('P', 0, 6),)),
    (4, (('P', 1, 4),)),
    (5, (('P', 0, 4),)),
    (6, (('P', 0, 1),)),
    (7, (('P', 1, 1),)),
    ('zo', 0),
    (4, (('P', 1, 3),)),
    (5, (('P', 0, 3),)),
    (6, (('P', 1, 3),)),
    (7, (('P', 0, 3),)),
    ('g', 5),
    (4, (('P', 0, 6),)),
    (5, (('P', 1, 6),)),
    ('ou', 6),
    ('oz', 7),
    ('zg', 0),
    ('z', 4),
    ('zo', 1),
    (0, (('P', 1, 7),)),
    (1, (('P', 0, 7),)),
    (2, (('P', 0, 3), ('P', 1, 5))),
    (3, (('P', 1, 3), ('P', 0, 5))),
    (6, (('P', 0, 6),)),
    (7, (('P', 1, 6),)),
    ('done', 0),
    ('ou', 7),
    ('zg', 1),
    (4, (('P', 1, 5),)),
    (5, (('P', 0, 5),)),
    ('z', 5),
    ('zg', 'V'),
    ('zf', 3),
    (5, (('P', 1, 7),)),
    ('done', 1),
    (2, (('P', 0, 4),)),
    (3, (('P', 1, 4),)),
    (4, (('P', 0, 7), ('P', 0, 4))),
    (5, (('P', 1, 4),)),
    (6, (('P', 0, 4),)),
    (7, (('P', 1, 4),)),
    ('zo', 'V'),
    (6, (('P', 0, 2),)),
    (7, (('P', 1, 2),)),
    ('o', 3),
    ('z', 6),
    ('o', 'V'),
    ('o', 5),
    ('zf', 5),
    ('done', 'V'),
    ('g', 6),
    (2, (('P', 0, 5),)),
    (3, (('P', 1, 5),)),
    (4, (('P', 1, 6),)),
    ('zg', 3),
    (5, (('P', 0, 6),)),
    ('zo', 2),
    (6, (('P', 0, 5),)),
    (7, (('P', 1, 7), ('P', 1, 5))),
    ('f', 6),
    (6, (('P', 0, 7),)),
    ('zf', 4),
    ('o', 4),
    ('done', 2),
    ('zg', 5),
    (4, (('P', 0, 5),)),
    (5, (('P', 1, 5),)),
    ('g', 7),
    (6, (('P', 0, 3),)),
    (7, (('P', 1, 3),)),
    ('z', 7),
    ('zg', 4),
    ('f', 7),
    ('zo', 3),
    ('zg', 6),
    (4, (('P', 1, 7),)),
    (5, (('P', 0, 7),)),
    ('zo', 5),
    (6, (('P', 1, 4),)),
    (7, (('P', 0, 4),)),
    ('done', 3),
    ('zf', 6),
    ('o', 6),
    ('done', 5),
    (6, (('P', 1, 5),)),
    (7, (('P', 0, 5),)),
    ('S', 0),
    ('zo', 4),
    ('zg', 7),
    ('zf', 7),
    ('o', 7),
    ('S', 1),
    ('done', 4),
    ('zo', 6),
    ('A', 0),
    ('A', 1),
    ('zo', 7),
    ('A', 2),
    ('done', 6),
    ('A', 3),
    ('done', 7),
    ('A', 5),
    ('A', 4),
    ('A', 6),
    ('A', 7),
    ('B', 0),
    ('B', 1),
    ('B', 2),
    ('B', 3),
    ('B', 5),
    ('B', 4),
    ('B', 6),
    ('B', 7),
)
ROUTE = {
    (0, 0): (0, {0: {0: ['y+', 'y-'], 3: ['y-']}, 1: {0: ['y+', 'y-'], 3: ['y-']}}),
    (0, 1): (0, {0: {0: ['y+', 'y-'], 3: ['y-']}, 1: {0: ['y+', 'y-'], 3: ['y-']}}),
    (0, 2): (0, {0: {0: ['y+', 'y-'], 3: ['y-']}, 1: {0: ['y+', 'y-'], 3: ['y-']}}),
    (0, 3): (0, {0: {0: ['y+', 'y-'], 3: ['y-']}, 1: {0: ['y+', 'y-'], 3: ['y-']}}),
    (0, 4): (1, {0: {0: ['y+', 'y-'], 3: ['y-']}, 1: {1: ['y-', 'y+'], 2: ['y+']}}),
    (0, 5): (1, {0: {0: ['y+', 'y-'], 3: ['y-']}, 1: {1: ['y-', 'y+'], 0: ['y-']}}),
    (0, 6): (3, {0: {0: ['y+', 'y-'], 3: ['y-']}, 1: {3: ['y-', 'y+'], 0: ['y+']}}),
    (0, 7): (3, {0: {0: ['y+', 'y-'], 3: ['y-']}, 1: {3: ['y-', 'y+'], 0: ['y+']}}),
    (1, 0): (1, {0: {1: ['y-', 'y+'], 2: ['y+']}, 1: {1: ['y-', 'y+'], 2: ['y+']}}),
    (1, 1): (1, {0: {1: ['y-', 'y+'], 2: ['y+']}, 1: {1: ['y-', 'y+'], 2: ['y+']}}),
    (1, 2): (1, {0: {1: ['y-', 'y+'], 2: ['y+']}, 1: {1: ['y-', 'y+'], 2: ['y+']}}),
    (1, 3): (1, {0: {1: ['y-', 'y+'], 2: ['y+']}, 1: {1: ['y-', 'y+'], 2: ['y+']}}),
    (1, 4): (0, {0: {1: ['y-', 'y+'], 2: ['y+']}, 1: {0: ['y+', 'y-'], 3: ['y-']}}),
    (1, 5): (0, {0: {1: ['y-', 'y+'], 2: ['y+']}, 1: {0: ['y+', 'y-'], 1: ['y+']}}),
    (1, 6): (2, {0: {1: ['y-', 'y+'], 2: ['y+']}, 1: {2: ['y+', 'y-'], 1: ['y-']}}),
    (1, 7): (2, {0: {1: ['y-', 'y+'], 2: ['y+']}, 1: {2: ['y+', 'y-'], 1: ['y-']}}),
}
Z, M, PL, O, ZM, ZP, ZO = range(7)


def kernel(m_hbm, l_hbm, d_hbm, out, solved, lbuf, pbuf, rbuf, vbuf, dbuf, acc,
           load_sem, l_recv, l_sib, l_send, v_recv, v_send, p_recv, r_recv, p_send):
    aux, pair = lax.axis_index("aux"), lax.axis_index("pair")
    zh, y = aux // 4, aux % 4
    zl, x, c = pair // 8, (pair // 2) % 4, pair % 2
    nb = l_hbm.shape[1]
    nrows = l_hbm.shape[2]
    nk = nb * 16
    nchunk = len(TYPES)
    piece = nk // NP
    half = piece // 2
    f32, bf16 = jnp.float32, jnp.bfloat16

    def at_pair(xx, zz, cc):
        return zz * 8 + lax.rem(xx + 8, 4) * 2 + cc

    sib = (aux, at_pair(x, zl, 1 - c))
    dev = {
        "x+": (aux, at_pair(x + 1, zl, c)),
        "x-": (aux, at_pair(x - 1, zl, c)),
        "y+": (zh * 4 + lax.rem(y + 1, 4), pair),
        "y-": (zh * 4 + lax.rem(y + 3, 4), pair),
        "zi": (aux, at_pair(x, 1 - zl, c)),
        "zo": ((1 - zh) * 4 + y, at_pair(x, 1 - zl, c)),
        "sib": sib,
    }

    own = pl.ds(pl.multiple_of(pair * nb, nb), nb)
    load_l = pltpu.make_async_copy(l_hbm, lbuf.at[:, own, :], load_sem.at[0])
    load_l.start()
    load_d = pltpu.make_async_copy(d_hbm, dbuf, load_sem.at[1])
    load_d.start()
    is_src = [aux == q for q in range(2)]
    load_p = [pltpu.make_async_copy(m_hbm.at[pl.ds(0, nk), :], pbuf.at[q], load_sem.at[2]) for q in range(2)]
    load_v = pltpu.make_async_copy(l_hbm.at[0, :, pl.ds(0, nk)], vbuf.at[own, :], load_sem.at[3])
    for q in range(2):
        pl.when(is_src[q])(load_p[q].start)
    pl.when(is_src[1])(load_v.start)
    load_m = pltpu.make_async_copy(m_hbm, out, load_sem.at[4])
    load_m.start()

    barrier = pltpu.get_barrier_semaphore()
    for d in dev.values():
        pl.semaphore_signal(barrier, inc=1, device_id=d, device_id_type=MESH)
    for k in range(1, 8):
        @pl.when(is_src[1])
        def _(k=k):
            pl.semaphore_signal(barrier, inc=1, device_id=(lax.rem(aux + k, 8), pair), device_id_type=MESH)

    @pl.when(jnp.logical_not(is_src[1]))
    def _():
        pl.semaphore_signal(barrier, inc=1, device_id=(1, pair), device_id_type=MESH)
        pl.semaphore_wait(barrier, 8)

    @pl.when(is_src[1])
    def _():
        pl.semaphore_wait(barrier, 14)

    def rows_of(r):
        start = r * CHUNK
        return pl.ds(start, min(CHUNK, nrows - start))

    def slot(r, first, count=nb):
        if r == "V":
            return vbuf.at[pl.ds(first, count), :]
        return lbuf.at[:, pl.ds(first, count), rows_of(r)]

    def index(r):
        return nchunk if r == "V" else r

    def kind(r):
        return "A" if r == "V" else TYPES[r]

    def parity(r):
        return 0 if r == "V" else TYPES[:r].count("B") % 2

    def message(r, xx, zz, to, sem):
        ref = slot(r, pl.multiple_of(at_pair(xx, zz, c) * nb, nb))
        return pltpu.make_async_remote_copy(ref, ref, l_send.at[index(r)], sem, device_id=to, device_id_type=MESH)

    def send(r, xx, zz, to, name):
        message(r, xx, zz, to, l_recv.at[index(r), name]).start()

    def sibling(r, xx, zz):
        message(r, xx, zz, sib, l_sib.at[index(r)]).start()

    def wait(r, xx, zz, name):
        message(r, xx, zz, sib, l_recv.at[index(r), name]).wait_recv()

    def sign(r, z_dyn):
        return z_dyn if kind(r) == "A" else lax.rem(z_dyn + parity(r), 2)

    def ev_oz(r):
        if r == "V":
            pl.when(jnp.logical_not(is_src[1]))(v_copy(1).wait_recv)
            ev_ou(r)
            ev_od(r)
        send(r, x, zl, dev["zi"], Z)

    def ev_ou(r):
        send(r, x, zl, dev["x+"], M)

    def ev_od(r):
        send(r, x, zl, dev["x-"], PL)
        sibling(r, x, zl)

    def across(r, xx, name):
        if kind(r) == "B":
            send(r, xx, zl, dev["zi"], name)

    def ev_f(r):
        s = sign(r, zl)
        step = 1 - 2 * s
        wait(r, x - step, zl, M + s)
        send(r, x - step, zl, (aux, at_pair(x + step, zl, c)), O)
        sibling(r, x - step, zl)
        across(r, x - step, ZM + s)

    def ev_g(r):
        s = sign(r, zl)
        step = 1 - 2 * s
        wait(r, x + step, zl, PL - s)
        sibling(r, x + step, zl)
        across(r, x + step, ZP - s)

    def ev_o(r):
        wait(r, x + 2, zl, O)
        sibling(r, x + 2, zl)
        across(r, x + 2, ZO)

    def ev_z(r):
        wait(r, x, 1 - zl, Z)
        if kind(r) == "A":
            send(r, x, 1 - zl, dev["x+"], ZM)
            send(r, x, 1 - zl, dev["x-"], ZP)
        sibling(r, x, 1 - zl)

    def ev_zf(r):
        s = sign(r, 1 - zl)
        step = 1 - 2 * s
        wait(r, x - step, 1 - zl, ZM + s)
        if kind(r) == "A":
            send(r, x - step, 1 - zl, (aux, at_pair(x + step, zl, c)), ZO)
        sibling(r, x - step, 1 - zl)

    def ev_zg(r):
        s = sign(r, 1 - zl)
        step = 1 - 2 * s
        wait(r, x + step, 1 - zl, ZP - s)
        sibling(r, x + step, 1 - zl)

    def ev_zo(r):
        wait(r, x + 2, 1 - zl, ZO)
        sibling(r, x + 2, 1 - zl)

    def ev_done(r):
        pltpu.make_async_remote_copy(slot(r, 0, 8 * nb), slot(r, 0, 8 * nb), l_send.at[index(r)], l_sib.at[index(r)],
                                     device_id=sib, device_id_type=MESH).wait_recv()

    def ev_sent(r):
        pltpu.make_async_remote_copy(slot(r, 0, 15 * nb), slot(r, 0, 15 * nb), l_send.at[index(r)], l_sib.at[index(r)],
                                     device_id=sib, device_id_type=MESH).wait_send()

    LINKS = ("y+", "y-", "zo", "zi")
    sent = {a: [] for a in range(8)}

    def p_copy(q, i, k, src, dst, to, sem):
        return pltpu.make_async_remote_copy(src, dst, p_send.at[q, i, k], sem, device_id=dev[to], device_id_type=MESH)

    def pivot(a, name, q, i):
        a_zh, a_y = a // 4, a % 4
        cross, trees = ROUTE[q, i]
        full = pbuf.at[q, pl.ds(i * piece, piece), :]
        first = pbuf.at[q, pl.ds(i * piece, half), :]
        second = pbuf.at[q, pl.ds(i * piece + half, half), :]
        relay = rbuf.at[q, pl.ds(i * half, half), :]
        got, rel = p_recv.at[q, i], r_recv.at[q, i]

        def go(k, src, dst, to, sem):
            copy = p_copy(q, i, k, src, dst, to, sem)
            copy.start()
            sent[a].append((q, i, k, src is full))

        if name == "P":
            p_copy(q, i, 0, full, full, "y+", got).wait_recv()
        if name == "X" or (name == "P" and a_zh == 0 and a_y == cross):
            go(2, second, relay, "zo", rel)
            go(3, first, relay, "zi", rel)
        if name[0] == "P":
            for link in trees[a_zh].get(a_y, ()):
                if name in ("P", "P" + link):
                    go(LINKS.index(link), full, full, link, got)
        if name == "R":
            p_copy(q, i, 4, relay, relay, "zi", rel).wait_recv()
            if a_zh == 0:
                go(4, relay, first, "zo", got)
            else:
                go(4, relay, second, "zi", got)

    def v_copy(k):
        ref = vbuf.at[own, :]
        return pltpu.make_async_remote_copy(ref, ref, v_send.at[k], v_recv.at[0], device_id=(lax.rem(aux + k, 8), pair), device_id_type=MESH)

    def ev_v():
        @pl.when(is_src[1])
        def _():
            load_v.wait()
            for k in range(1, 8):
                v_copy(k).start()

    def halves(v):
        h = v.astype(bf16)
        return h, (v - h.astype(f32)).astype(bf16)

    def dot(a, b):
        return jnp.dot(a, b, preferred_element_type=f32)

    def dot_t(a, b):
        return lax.dot_general(a, b, (((0,), (0,)), ((), ())), preferred_element_type=f32)

    width = 256
    cols = [pl.ds(n * width, width) for n in range(out.shape[1] // width)]

    def solve(q):
        dh, dl = halves(dbuf[q])
        for n in cols:
            if q == 0:
                p = pbuf[0, :, n]
                s = dot(dh, p) + dot(dl, p)
            else:
                w = pbuf[1, :, n].astype(f32) - dot_t(vbuf[...], solved[0, :, n])
                wh, wl = halves(w)
                s = dot(dh, wh) + dot(dl, wh) + dot(dh, wl)
            solved[q, :, n] = s.astype(bf16)

    def product(rows, q, last):
        lq = [lbuf[k, :, rows] for k in range(q, last + 1)]
        for n in cols:
            o = out[rows, n].astype(f32) if q == 0 else acc[rows, n]
            for k in range(q, last + 1):
                o = o - dot_t(lq[k - q], solved[k, :, n])
            if last == 1:
                out[rows, n] = o.astype(bf16)
            else:
                acc[rows, n] = o

    load_l.wait()
    for q in range(2):
        pl.when(is_src[q])(load_p[q].wait)
    ev_v()
    act = {"oz": ev_oz, "ou": ev_ou, "od": ev_od, "z": ev_z, "f": ev_f, "g": ev_g, "o": ev_o,
           "zf": ev_zf, "zg": ev_zg, "zo": ev_zo, "done": ev_done}
    chunks = ["V"] + list(range(nchunk))
    skip = False
    for n, step in enumerate(ORDER):
        name, r = step
        if name in act:
            act[name](r)
        elif name == "S":
            if r == 0:
                load_d.wait()
                load_m.wait()
            solve(r)
        elif name == "A":
            skip = n + 1 < len(ORDER) and ORDER[n + 1] == ("B", r)
            product(rows_of(r), 0, 1 if skip else 0)
        elif name == "B":
            if not skip:
                product(rows_of(r), 1, 1)
            skip = False
        else:
            @pl.when(aux == name)
            def _(a=name, todo=r):
                for what, q, i in todo:
                    pivot(a, what, q, i)

    for r in chunks:
        ev_sent(r)
    for a in sent:
        @pl.when(aux == a)
        def _(a=a):
            for q, i, k, whole in sent[a]:
                ref = pbuf.at[q, pl.ds(i * piece, piece if whole else half), :]
                p_copy(q, i, k, ref, ref, "y+", p_recv.at[q, i]).wait_send()

    @pl.when(is_src[1])
    def _():
        for k in range(1, 8):
            v_copy(k).wait_send()


def solution(mesh):
    def step(m_panels, lower_cols, diag_inverses):
        rows, cols = m_panels.shape
        panels, nk, _ = diag_inverses.shape
        dma = pltpu.SemaphoreType.DMA
        n = len(TYPES) + 1
        out, solved = pl.pallas_call(
            kernel,
            out_shape=(
                pltpu.VMEM((rows, cols), jnp.bfloat16),
                pltpu.VMEM((panels, nk, cols), jnp.bfloat16),
            ),
            in_specs=[pl.BlockSpec(memory_space=pltpu.HBM)] * 3,
            out_specs=(pl.BlockSpec(memory_space=pltpu.VMEM),) * 2,
            scratch_shapes=[
                pltpu.VMEM((panels, nk, rows), jnp.bfloat16),
                pltpu.VMEM((panels, nk, cols), jnp.bfloat16),
                pltpu.VMEM((panels, nk // 2, cols), jnp.bfloat16),
                pltpu.VMEM((nk, nk), jnp.bfloat16),
                pltpu.VMEM((panels, nk, nk), jnp.float32),
                pltpu.VMEM((rows, cols), jnp.float32),
                dma((5,)), dma((n, 7)), dma((n,)), dma((n,)), dma((1,)), dma((8,)),
                dma((panels, NP)), dma((panels, NP)), dma((panels, NP, 5)),
            ],
            compiler_params=pltpu.CompilerParams(collective_id=0, has_side_effects=True, vmem_limit_bytes=46 * 2**20),
        )(m_panels, lower_cols, diag_inverses)
        return out, solved

    return jax.shard_map(
        step,
        mesh=mesh,
        in_specs=(P("aux", "pair"), P(None, "pair", "aux"), P()),
        out_specs=(P("aux", "pair"), P(None, None, "pair")),
        check_vma=False,
    )
```

```python
import functools

import jax
import jax.numpy as jnp
from jax import lax
from jax.experimental import pallas as pl
from jax.experimental.pallas import tpu as pltpu
from jax.sharding import PartitionSpec as P

MESH = pl.DeviceIdType.MESH
TYPES = "AABAABAA"
NP = 8
ORDER = (
    (0, (('Py+', 0, 1), ('Py+', 0, 0), ('Py-', 0, 0), ('Py-', 0, 3), ('X', 0, 5), ('X', 0, 6), ('X', 0, 7))),
    (1, (('Py+', 1, 0), ('Py+', 1, 2), ('Py-', 1, 0), ('Py-', 1, 1), ('X', 1, 4), ('X', 1, 6), ('X', 1, 7))),
    ('od', 0),
    ('od', 1),
    ('od', 2),
    ('od', 3),
    ('od', 4),
    ('od', 5),
    ('od', 6),
    ('od', 7),
    ('ou', 0),
    ('ou', 1),
    ('oz', 0),
    ('ou', 2),
    ('oz', 1),
    (0, (('Py+', 0, 2), ('Py-', 0, 4), ('R', 0, 5))),
    (1, (('Py+', 1, 3), ('Py-', 1, 3), ('R', 1, 4))),
    (4, (('R', 0, 5),)),
    (5, (('R', 1, 4),)),
    ('oz', 2),
    ('g', 0),
    ('f', 0),
    ('oz', 'V'),
    (0, (('P', 1, 0), ('R', 0, 6), ('Py+', 0, 3))),
    (1, (('R', 1, 6), ('P', 0, 0), ('Py-', 1, 4))),
    (2, (('P', 1, 0),)),
    (3, (('P', 0, 0),)),
    (4, (('R', 0, 6),)),
    (5, (('R', 1, 6),)),
    ('f', 1),
    ('g', 1),
    (0, (('R', 0, 7), ('P', 1, 1), ('Py+', 0, 4), ('Py-', 0, 5))),
    (1, (('R', 1, 7), ('P', 0, 1), ('Py-', 1, 5))),
    (2, (('P', 1, 2),)),
    (3, (('P', 0, 3),)),
    (4, (('R', 0, 7),)),
    (5, (('R', 1, 7),)),
    ('z', 0),
    ('g', 2),
    ('f', 2),
    (4, (('P', 0, 5),)),
    (5, (('P', 1, 4),)),
    (6, (('R', 1, 0),)),
    (7, (('R', 0, 0),)),
    ('z', 1),
    (0, (('P', 1, 3), ('Py+', 0, 5))),
    (1, (('P', 0, 2), ('Py+', 1, 5), ('Py-', 1, 7))),
    (2, (('R', 1, 0), ('P', 0, 0), ('P', 1, 3))),
    (3, (('R', 0, 0), ('P', 0, 4))),
    ('ou', 3),
    ('oz', 3),
    (1, (('P', 0, 3),)),
    (2, (('R', 1, 2),)),
    (3, (('R', 0, 3), ('P', 1, 2))),
    (4, (('P', 0, 6), ('R', 1, 1))),
    (5, (('P', 1, 6), ('R', 0, 1))),
    (6, (('R', 1, 2),)),
    (7, (('R', 0, 3),)),
    ('z', 2),
    ('z', 'V'),
    (0, (('P', 1, 4), ('Py+', 0, 6), ('R', 1, 1))),
    (1, (('Py+', 1, 6), ('R', 0, 1))),
    (2, (('P', 0, 3), ('P', 0, 1))),
    (3, (('P', 1, 1),)),
    (4, (('P', 0, 7),)),
    (5, (('P', 1, 7), ('R', 0, 2))),
    (6, (('P', 1, 4),)),
    ('ou', 4),
    (3, (('P', 1, 3),)),
    (4, (('P', 1, 4),)),
    (5, (('P', 0, 5),)),
    (6, (('R', 1, 3),)),
    (7, (('P', 0, 5), ('R', 0, 4))),
    ('g', 3),
    ('oz', 4),
    (0, (('P', 1, 5), ('Py+', 0, 7), ('Py-', 0, 6))),
    (1, (('Py+', 1, 7),)),
    (2, (('P', 0, 4), ('P', 0, 2))),
    (3, (('P', 1, 0), ('P', 0, 5))),
    (5, (('P', 0, 6),)),
    ('g', 'V'),
    (1, (('P', 0, 4),)),
    ('zg', 2),
    (6, (('P', 1, 0), ('P', 1, 6))),
    (7, (('P', 0, 0),)),
    ('o', 0),
    (2, (('R', 1, 3),)),
    (3, (('R', 0, 4),)),
    (7, (('P', 0, 6),)),
    ('zf', 0),
    ('f', 'V'),
    ('ou', 5),
    (0, (('P', 1, 2),)),
    ('oz', 5),
    (0, (('P', 1, 7), ('Py-', 0, 7))),
    (1, (('P', 0, 5),)),
    (2, (('P', 1, 1), ('P', 1, 5))),
    (3, (('P', 0, 1), ('P', 1, 4))),
    (4, (('P', 1, 7),)),
    ('zf', 1),
    ('zf', 2),
    (7, (('P', 0, 3),)),
    ('g', 4),
    ('f', 3),
    (1, (('R', 0, 2),)),
    (5, (('P', 0, 7),)),
    (6, (('P', 1, 2), ('P', 0, 5))),
    (7, (('P', 1, 4), ('P', 0, 7))),
    ('zf', 'V'),
    (2, (('P', 0, 5),)),
    (3, (('P', 0, 2),)),
    (4, (('P', 1, 1),)),
    (5, (('P', 0, 1),)),
    ('zg', 0),
    (1, (('P', 0, 6),)),
    (2, (('P', 1, 6),)),
    (3, (('P', 1, 5),)),
    (4, (('P', 0, 0),)),
    (5, (('P', 1, 0),)),
    (6, (('P', 0, 0),)),
    (7, (('P', 0, 4),)),
    ('z', 3),
    ('f', 4),
    ('zo', 0),
    (7, (('P', 1, 0),)),
    ('o', 1),
    (6, (('P', 1, 3), ('R', 1, 5))),
    ('ou', 6),
    (6, (('P', 0, 6),)),
    ('done', 0),
    (7, (('P', 1, 7),)),
    ('z', 4),
    ('o', 2),
    (1, (('P', 0, 7),)),
    (2, (('P', 1, 4),)),
    (3, (('P', 0, 6),)),
    ('f', 5),
    (2, (('R', 1, 5),)),
    (4, (('P', 0, 3),)),
    (5, (('P', 0, 2), ('P', 1, 2))),
    (6, (('P', 0, 3),)),
    ('g', 5),
    (7, (('P', 1, 6),)),
    ('zg', 1),
    (4, (('P', 0, 1),)),
    ('zo', 1),
    (5, (('P', 1, 1),)),
    (6, (('P', 0, 7),)),
    (7, (('P', 1, 1),)),
    ('done', 1),
    ('o', 'V'),
    ('zg', 'V'),
    ('oz', 6),
    (2, (('P', 1, 7),)),
    ('zo', 'V'),
    (3, (('P', 1, 6), ('P', 0, 7))),
    ('ou', 7),
    (4, (('P', 0, 4),)),
    ('oz', 7),
    (5, (('P', 1, 3),)),
    (6, (('P', 0, 4),)),
    ('z', 5),
    (7, (('P', 1, 2),)),
    ('zf', 3),
    (5, (('P', 0, 0),)),
    (6, (('P', 0, 1),)),
    ('o', 3),
    ('zo', 2),
    (2, (('P', 0, 7), ('P', 0, 6))),
    (3, (('P', 1, 7),)),
    (4, (('P', 0, 2),)),
    (6, (('P', 1, 5),)),
    ('zf', 4),
    (0, (('P', 1, 6),)),
    (4, (('P', 1, 0),)),
    ('zg', 3),
    ('done', 2),
    (5, (('P', 0, 3),)),
    (6, (('P', 1, 7), ('P', 0, 2))),
    (7, (('P', 1, 3), ('P', 0, 1))),
    ('g', 6),
    ('o', 4),
    ('done', 'V'),
    ('f', 6),
    ('o', 5),
    (4, (('P', 1, 6), ('P', 1, 3))),
    (6, (('P', 1, 1),)),
    ('f', 7),
    ('zg', 4),
    ('zg', 5),
    ('g', 7),
    ('zf', 5),
    ('z', 6),
    (5, (('P', 0, 4),)),
    (7, (('P', 0, 2),)),
    ('S', 0),
    (7, (('P', 1, 5),)),
    ('z', 7),
    (4, (('P', 1, 2),)),
    ('zo', 3),
    (5, (('P', 1, 5),)),
    ('A', 0),
    ('o', 6),
    ('A', 1),
    ('zo', 4),
    ('done', 3),
    ('o', 7),
    ('zf', 6),
    ('A', 2),
    ('zo', 5),
    ('zg', 6),
    ('A', 3),
    ('zg', 7),
    ('done', 4),
    ('zf', 7),
    ('A', 4),
    ('zo', 6),
    (4, (('P', 1, 5),)),
    ('S', 1),
    ('zo', 7),
    ('done', 6),
    ('done', 5),
    ('B', 0),
    ('done', 7),
    ('B', 1),
    ('B', 2),
    ('B', 3),
    ('B', 4),
)
ROUTE = {
    (0, 0): (3, {0: {0: ['y+', 'y-'], 3: ['y-']}, 1: {3: ['y+', 'y-'], 0: ['y+']}}),
    (0, 1): (1, {0: {0: ['y+'], 1: ['y+'], 2: ['y+']}, 1: {1: ['y+', 'y-'], 0: ['y-']}}),
    (0, 2): (1, {0: {0: ['y+'], 1: ['y+'], 2: ['y+']}, 1: {1: ['y+', 'y-'], 0: ['y-']}}),
    (0, 3): (3, {0: {0: ['y+', 'y-'], 3: ['y-']}, 1: {3: ['y+', 'y-'], 0: ['y+']}}),
    (0, 4): (3, {0: {0: ['y+', 'y-'], 3: ['y-']}, 1: {3: ['y+', 'y-'], 2: ['y-']}}),
    (0, 5): (0, {0: {0: ['y+', 'y-'], 3: ['y-']}, 1: {0: ['y+', 'y-'], 1: ['y+']}}),
    (0, 6): (0, {0: {0: ['y+', 'y-'], 3: ['y-']}, 1: {0: ['y+', 'y-'], 1: ['y+']}}),
    (0, 7): (0, {0: {0: ['y+', 'y-'], 1: ['y+']}, 1: {0: ['y+', 'y-'], 1: ['y+']}}),
    (1, 0): (2, {0: {1: ['y+', 'y-'], 2: ['y+']}, 1: {2: ['y+', 'y-'], 3: ['y+']}}),
    (1, 1): (0, {0: {1: ['y-'], 0: ['y-'], 3: ['y-']}, 1: {0: ['y+', 'y-'], 3: ['y-']}}),
    (1, 2): (2, {0: {1: ['y+'], 2: ['y+'], 3: ['y+']}, 1: {2: ['y+', 'y-'], 3: ['y+']}}),
    (1, 3): (2, {0: {1: ['y+', 'y-'], 2: ['y+']}, 1: {2: ['y+', 'y-'], 1: ['y-']}}),
    (1, 4): (1, {0: {1: ['y-'], 0: ['y-'], 3: ['y-']}, 1: {1: ['y+', 'y-'], 2: ['y+']}}),
    (1, 5): (2, {0: {1: ['y+', 'y-'], 0: ['y-']}, 1: {2: ['y+', 'y-'], 1: ['y-']}}),
    (1, 6): (1, {0: {1: ['y+'], 2: ['y+'], 3: ['y+']}, 1: {1: ['y+'], 2: ['y+'], 3: ['y+']}}),
    (1, 7): (1, {0: {1: ['y+', 'y-'], 2: ['y+']}, 1: {1: ['y-'], 0: ['y-'], 3: ['y-']}}),
}
CHUNKS = ((0, 640), (640, 640), (1280, 896), (2176, 640), (2816, 640), (3456, 896), (4352, 384), (4736, 264))
TAIL = (5, 6, 7)
Z, M, PL, O, ZM, ZP, ZO = range(7)


def kernel(m_hbm, l_hbm, d_hbm, out, solved, lbuf, pbuf, rbuf, vbuf, dbuf, acc,
           load_sem, l_recv, l_sib, l_send, v_recv, v_send, p_recv, r_recv, p_send):
    aux, pair = lax.axis_index("aux"), lax.axis_index("pair")
    zh, y = aux // 4, aux % 4
    zl, x, c = pair // 8, (pair // 2) % 4, pair % 2
    nb = l_hbm.shape[1]
    nrows = l_hbm.shape[2]
    nk = nb * 16
    nchunk = len(TYPES)
    piece = nk // NP
    half = piece // 2
    f32, bf16 = jnp.float32, jnp.bfloat16

    def at_pair(xx, zz, cc):
        return zz * 8 + lax.rem(xx + 8, 4) * 2 + cc

    sib = (aux, at_pair(x, zl, 1 - c))
    dev = {
        "x+": (aux, at_pair(x + 1, zl, c)),
        "x-": (aux, at_pair(x - 1, zl, c)),
        "y+": (zh * 4 + lax.rem(y + 1, 4), pair),
        "y-": (zh * 4 + lax.rem(y + 3, 4), pair),
        "zi": (aux, at_pair(x, 1 - zl, c)),
        "zo": ((1 - zh) * 4 + y, at_pair(x, 1 - zl, c)),
        "sib": sib,
    }

    own = pl.ds(pl.multiple_of(pair * nb, nb), nb)
    load_l = pltpu.make_async_copy(l_hbm, lbuf.at[:, own, :], load_sem.at[0])
    load_l.start()
    load_d = pltpu.make_async_copy(d_hbm, dbuf, load_sem.at[1])
    load_d.start()
    is_src = [aux == q for q in range(2)]
    load_p = [pltpu.make_async_copy(m_hbm.at[pl.ds(0, nk), :], pbuf.at[q], load_sem.at[2]) for q in range(2)]
    load_v = pltpu.make_async_copy(l_hbm.at[0, :, pl.ds(0, nk)], vbuf.at[own, :], load_sem.at[3])
    for q in range(2):
        pl.when(is_src[q])(load_p[q].start)
    pl.when(is_src[1])(load_v.start)
    load_m = pltpu.make_async_copy(m_hbm, out, load_sem.at[4])
    load_m.start()

    barrier = pltpu.get_barrier_semaphore()
    for d in dev.values():
        pl.semaphore_signal(barrier, inc=1, device_id=d, device_id_type=MESH)
    for k in range(1, 8):
        @pl.when(is_src[1])
        def _(k=k):
            pl.semaphore_signal(barrier, inc=1, device_id=(lax.rem(aux + k, 8), pair), device_id_type=MESH)

    @pl.when(jnp.logical_not(is_src[1]))
    def _():
        pl.semaphore_signal(barrier, inc=1, device_id=(1, pair), device_id_type=MESH)
        pl.semaphore_wait(barrier, 8)

    @pl.when(is_src[1])
    def _():
        pl.semaphore_wait(barrier, 14)

    def rows_of(r):
        return pl.ds(*CHUNKS[r])

    def slot(r, first, count=nb):
        if r == "V":
            return vbuf.at[pl.ds(first, count), :]
        return lbuf.at[:, pl.ds(first, count), rows_of(r)]

    def index(r):
        return nchunk if r == "V" else r

    def kind(r):
        return "A" if r == "V" else TYPES[r]

    def parity(r):
        return 0 if r == "V" else TYPES[:r].count("B") % 2

    def message(r, xx, zz, to, sem):
        ref = slot(r, pl.multiple_of(at_pair(xx, zz, c) * nb, nb))
        return pltpu.make_async_remote_copy(ref, ref, l_send.at[index(r)], sem, device_id=to, device_id_type=MESH)

    def send(r, xx, zz, to, name):
        message(r, xx, zz, to, l_recv.at[index(r), name]).start()

    def sibling(r, xx, zz):
        message(r, xx, zz, sib, l_sib.at[index(r)]).start()

    def wait(r, xx, zz, name):
        message(r, xx, zz, sib, l_recv.at[index(r), name]).wait_recv()

    def sign(r, z_dyn):
        return z_dyn if kind(r) == "A" else lax.rem(z_dyn + parity(r), 2)

    def ev_oz(r):
        if r == "V":
            pl.when(jnp.logical_not(is_src[1]))(v_copy(1).wait_recv)
            ev_ou(r)
            ev_od(r)
        send(r, x, zl, dev["zi"], Z)

    def ev_ou(r):
        send(r, x, zl, dev["x+"], M)

    def ev_od(r):
        send(r, x, zl, dev["x-"], PL)
        sibling(r, x, zl)

    def across(r, xx, name):
        if kind(r) == "B":
            send(r, xx, zl, dev["zi"], name)

    def ev_f(r):
        s = sign(r, zl)
        step = 1 - 2 * s
        wait(r, x - step, zl, M + s)
        send(r, x - step, zl, (aux, at_pair(x + step, zl, c)), O)
        sibling(r, x - step, zl)
        across(r, x - step, ZM + s)

    def ev_g(r):
        s = sign(r, zl)
        step = 1 - 2 * s
        wait(r, x + step, zl, PL - s)
        sibling(r, x + step, zl)
        across(r, x + step, ZP - s)

    def ev_o(r):
        wait(r, x + 2, zl, O)
        sibling(r, x + 2, zl)
        across(r, x + 2, ZO)

    def ev_z(r):
        wait(r, x, 1 - zl, Z)
        if kind(r) == "A":
            send(r, x, 1 - zl, dev["x+"], ZM)
            send(r, x, 1 - zl, dev["x-"], ZP)
        sibling(r, x, 1 - zl)

    def ev_zf(r):
        s = sign(r, 1 - zl)
        step = 1 - 2 * s
        wait(r, x - step, 1 - zl, ZM + s)
        if kind(r) == "A":
            send(r, x - step, 1 - zl, (aux, at_pair(x + step, zl, c)), ZO)
        sibling(r, x - step, 1 - zl)

    def ev_zg(r):
        s = sign(r, 1 - zl)
        step = 1 - 2 * s
        wait(r, x + step, 1 - zl, ZP - s)
        sibling(r, x + step, 1 - zl)

    def ev_zo(r):
        wait(r, x + 2, 1 - zl, ZO)
        sibling(r, x + 2, 1 - zl)

    def ev_done(r):
        pltpu.make_async_remote_copy(slot(r, 0, 8 * nb), slot(r, 0, 8 * nb), l_send.at[index(r)], l_sib.at[index(r)],
                                     device_id=sib, device_id_type=MESH).wait_recv()

    def ev_sent(r):
        pltpu.make_async_remote_copy(slot(r, 0, 15 * nb), slot(r, 0, 15 * nb), l_send.at[index(r)], l_sib.at[index(r)],
                                     device_id=sib, device_id_type=MESH).wait_send()

    LINKS = ("y+", "y-", "zo", "zi")
    sent = {a: [] for a in range(8)}

    def p_copy(q, i, k, src, dst, to, sem):
        return pltpu.make_async_remote_copy(src, dst, p_send.at[q, i, k], sem, device_id=dev[to], device_id_type=MESH)

    def pivot(a, name, q, i):
        a_zh, a_y = a // 4, a % 4
        cross, trees = ROUTE[q, i]
        full = pbuf.at[q, pl.ds(i * piece, piece), :]
        first = pbuf.at[q, pl.ds(i * piece, half), :]
        second = pbuf.at[q, pl.ds(i * piece + half, half), :]
        relay = rbuf.at[q, pl.ds(i * half, half), :]
        got, rel = p_recv.at[q, i], r_recv.at[q, i]

        def go(k, src, dst, to, sem):
            copy = p_copy(q, i, k, src, dst, to, sem)
            copy.start()
            sent[a].append((q, i, k, src is full))

        if name == "P":
            p_copy(q, i, 0, full, full, "y+", got).wait_recv()
        if name == "X" or (name == "P" and a_zh == 0 and a_y == cross):
            go(2, second, relay, "zo", rel)
            go(3, first, relay, "zi", rel)
        if name[0] == "P":
            for link in trees[a_zh].get(a_y, ()):
                if name in ("P", "P" + link):
                    go(LINKS.index(link), full, full, link, got)
        if name == "R":
            p_copy(q, i, 4, relay, relay, "zi", rel).wait_recv()
            if a_zh == 0:
                go(4, relay, first, "zo", got)
            else:
                go(4, relay, second, "zi", got)

    def v_copy(k):
        ref = vbuf.at[own, :]
        return pltpu.make_async_remote_copy(ref, ref, v_send.at[k], v_recv.at[0], device_id=(lax.rem(aux + k, 8), pair), device_id_type=MESH)

    def ev_v():
        @pl.when(is_src[1])
        def _():
            load_v.wait()
            for k in range(1, 8):
                v_copy(k).start()

    def halves(v):
        h = v.astype(bf16)
        return h, (v - h.astype(f32)).astype(bf16)

    def dot(a, b):
        return jnp.dot(a, b, preferred_element_type=f32)

    def dot_t(a, b):
        return lax.dot_general(a, b, (((0,), (0,)), ((), ())), preferred_element_type=f32)

    width = 256
    cols = [pl.ds(n * width, width) for n in range(out.shape[1] // width)]

    def solve(q):
        dh, dl = halves(dbuf[q])
        for n in cols:
            if q == 0:
                p = pbuf[0, :, n]
                s = dot(dh, p) + dot(dl, p)
            else:
                w = pbuf[1, :, n].astype(f32) - dot_t(vbuf[...], solved[0, :, n])
                wh, wl = halves(w)
                s = dot(dh, wh) + dot(dl, wh) + dot(dh, wl)
            solved[q, :, n] = s.astype(bf16)

    def product(rows, q, last):
        lq = [lbuf[k, :, rows] for k in range(q, last + 1)]
        for n in cols:
            o = out[rows, n].astype(f32) if q == 0 else acc[rows, n]
            for k in range(q, last + 1):
                o = o - dot_t(lq[k - q], solved[k, :, n])
            if last == 1:
                out[rows, n] = o.astype(bf16)
            else:
                acc[rows, n] = o

    load_l.wait()
    for q in range(2):
        pl.when(is_src[q])(load_p[q].wait)
    ev_v()
    act = {"oz": ev_oz, "ou": ev_ou, "od": ev_od, "z": ev_z, "f": ev_f, "g": ev_g, "o": ev_o,
           "zf": ev_zf, "zg": ev_zg, "zo": ev_zo, "done": ev_done}
    chunks = ["V"] + list(range(nchunk))
    skip = False
    for n, step in enumerate(ORDER):
        name, r = step
        if name in act:
            act[name](r)
        elif name == "S":
            if r == 0:
                load_d.wait()
                load_m.wait()
            solve(r)
        elif name == "A":
            skip = ("B", r) == (ORDER + ((),))[n + 1]
            product(rows_of(r), 0, 1 if skip else 0)
        elif name == "B":
            if not skip:
                product(rows_of(r), 1, 1)
            skip = False
        else:
            @pl.when(aux == name)
            def _(a=name, todo=r):
                for what, q, i in todo:
                    pivot(a, what, q, i)

    for r in chunks:
        ev_sent(r)
    for a in sent:
        @pl.when(aux == a)
        def _(a=a):
            for q, i, k, whole in sent[a]:
                ref = pbuf.at[q, pl.ds(i * piece, piece if whole else half), :]
                p_copy(q, i, k, ref, ref, "y+", p_recv.at[q, i]).wait_send()

    @pl.when(is_src[1])
    def _():
        for k in range(1, 8):
            v_copy(k).wait_send()


def finish(part, lbuf, solved, out_hbm, solved_hbm, late, sems):
    f32, bf16 = jnp.float32, jnp.bfloat16
    n_sem = iter(range(2 + len(CHUNKS)))
    copies = [pltpu.make_async_copy(solved, solved_hbm, sems.at[next(n_sem)])]
    ready = sorted(CHUNKS[r] for r in range(len(CHUNKS)) if r not in TAIL)
    runs = []
    for start, size in ready:
        if runs and runs[-1][0] + runs[-1][1] == start:
            runs[-1][1] += size
        else:
            runs.append([start, size])
    for start, size in runs:
        rows = pl.ds(start, size)
        copies.append(pltpu.make_async_copy(part.at[rows, :], out_hbm.at[rows, :], sems.at[next(n_sem)]))
    for copy in copies:
        copy.start()
    base = 0
    width = 256
    for r in TAIL:
        start, size = CHUNKS[r]
        rows = pl.ds(start, size)
        lq = [lbuf[k, :, rows] for k in range(2)]
        for c in range(part.shape[1] // width):
            n = pl.ds(c * width, width)
            o = part[rows, n].astype(f32)
            for k in range(2):
                o = o - lax.dot_general(lq[k], solved[k, :, n], (((0,), (0,)), ((), ())), preferred_element_type=f32)
            late[pl.ds(base, size), n] = o.astype(bf16)
        copy = pltpu.make_async_copy(late.at[pl.ds(base, size), :], out_hbm.at[rows, :], sems.at[next(n_sem)])
        copy.start()
        copies.append(copy)
        base += size
    for copy in copies:
        copy.wait()


def solution(mesh):
    def step(m_panels, lower_cols, diag_inverses):
        rows, cols = m_panels.shape
        panels, nk, _ = diag_inverses.shape
        dma = pltpu.SemaphoreType.DMA
        n = len(TYPES) + 1
        bf16 = jnp.bfloat16
        part, solved, lbuf = pl.pallas_call(
            kernel,
            out_shape=(
                pltpu.VMEM((rows, cols), bf16),
                pltpu.VMEM((panels, nk, cols), bf16),
                pltpu.VMEM((panels, nk, rows), bf16),
            ),
            in_specs=[pl.BlockSpec(memory_space=pltpu.HBM)] * 3,
            out_specs=(pl.BlockSpec(memory_space=pltpu.VMEM),) * 3,
            scratch_shapes=[
                pltpu.VMEM((panels, nk, cols), bf16),
                pltpu.VMEM((panels, nk // 2, cols), bf16),
                pltpu.VMEM((nk, nk), bf16),
                pltpu.VMEM((panels, nk, nk), jnp.float32),
                pltpu.VMEM((rows, cols), jnp.float32),
                dma((5,)), dma((n, 7)), dma((n,)), dma((n,)), dma((1,)), dma((8,)),
                dma((panels, NP)), dma((panels, NP)), dma((panels, NP, 5)),
            ],
            compiler_params=pltpu.CompilerParams(collective_id=0, has_side_effects=True, vmem_limit_bytes=36 * 2**20),
        )(m_panels, lower_cols, diag_inverses)
        late = -(-sum(CHUNKS[r][1] for r in TAIL) // 16) * 16
        return pl.pallas_call(
            finish,
            out_shape=(jax.ShapeDtypeStruct((rows, cols), bf16), jax.ShapeDtypeStruct((panels, nk, cols), bf16)),
            in_specs=[pl.BlockSpec(memory_space=pltpu.VMEM)] * 3,
            out_specs=(pl.BlockSpec(memory_space=pltpu.HBM),) * 2,
            scratch_shapes=[pltpu.VMEM((late, cols), bf16), dma((2 + len(CHUNKS),))],
            compiler_params=pltpu.CompilerParams(vmem_limit_bytes=12 * 2**20),
        )(*(pltpu.with_memory_space_constraint(v, pltpu.VMEM) for v in (part, lbuf, solved)))

    return jax.shard_map(
        step,
        mesh=mesh,
        in_specs=(P("aux", "pair"), P(None, "pair", "aux"), P()),
        out_specs=(P("aux", "pair"), P(None, None, "pair")),
        check_vma=False,
    )
```

```python
import functools

import jax
import jax.numpy as jnp
from jax import lax
from jax.experimental import pallas as pl
from jax.experimental.pallas import tpu as pltpu
from jax.sharding import PartitionSpec as P

MESH = pl.DeviceIdType.MESH
TYPES = "AABAABAA"
NP = 8
ORDER = (
    ('ou', 0),
    (0, (('X', 0, 6), ('Py+', 0, 0), ('Py+', 0, 1), ('Py-', 0, 0), ('Py-', 0, 3))),
    (1, (('Py-', 1, 0), ('Py+', 1, 0), ('Py+', 1, 2), ('Py-', 1, 1), ('X', 1, 4), ('X', 1, 6), ('X', 1, 7))),
    ('od', 0),
    ('od', 1),
    ('od', 2),
    ('od', 4),
    ('od', 5),
    ('od', 6),
    ('od', 7),
    ('ou', 1),
    (0, (('X', 0, 5),)),
    ('ou', 2),
    (0, (('X', 0, 7),)),
    ('oz', 1),
    ('oz', 0),
    ('od', 3),
    ('oz', 2),
    (0, (('Py+', 0, 2), ('Py-', 0, 4), ('R', 0, 5))),
    (1, (('Py-', 1, 3), ('Py+', 1, 3), ('Py+', 1, 5), ('R', 1, 4))),
    (4, (('R', 0, 5),)),
    (5, (('R', 1, 4),)),
    ('g', 0),
    ('f', 0),
    (0, (('P', 1, 0), ('R', 0, 6), ('Py+', 0, 3), ('Py-', 0, 5))),
    (1, (('P', 0, 0), ('R', 1, 6), ('Py-', 1, 4))),
    (2, (('P', 1, 0),)),
    (3, (('P', 0, 0),)),
    (4, (('R', 0, 6),)),
    (5, (('R', 1, 6),)),
    ('f', 1),
    (0, (('R', 0, 7),)),
    (1, (('R', 1, 7),)),
    (4, (('R', 0, 7),)),
    (5, (('R', 1, 7), ('P', 1, 4))),
    ('oz', 'V'),
    ('g', 2),
    ('f', 2),
    (0, (('P', 1, 1),)),
    (1, (('P', 0, 1),)),
    (2, (('P', 1, 2),)),
    (3, (('P', 0, 3),)),
    ('oz', 3),
    (0, (('Py+', 0, 4),)),
    (1, (('Py+', 1, 6), ('Py-', 1, 5))),
    ('g', 1),
    (4, (('P', 0, 5),)),
    (6, (('R', 1, 0),)),
    (7, (('R', 0, 0),)),
    ('z', 0),
    (0, (('Py-', 0, 6),)),
    (2, (('R', 1, 0),)),
    ('ou', 3),
    ('z', 1),
    (0, (('Py+', 0, 5), ('P', 1, 3), ('Py-', 0, 7))),
    (1, (('P', 0, 2), ('Py+', 1, 7), ('Py-', 1, 7))),
    (2, (('P', 0, 0), ('P', 1, 3))),
    (3, (('P', 0, 4),)),
    (4, (('P', 0, 6),)),
    (5, (('P', 1, 6),)),
    ('ou', 4),
    ('z', 2),
    (3, (('R', 0, 0),)),
    (4, (('R', 1, 1), ('P', 0, 7))),
    (5, (('R', 0, 1),)),
    (6, (('R', 1, 2),)),
    (7, (('R', 0, 3),)),
    ('z', 'V'),
    (5, (('P', 1, 7), ('R', 0, 2))),
    ('zg', 2),
    (2, (('P', 0, 3),)),
    (3, (('P', 1, 2),)),
    ('oz', 4),
    (0, (('P', 1, 4), ('Py+', 0, 6))),
    (1, (('P', 0, 3),)),
    (2, (('P', 1, 5),)),
    (3, (('P', 0, 5),)),
    (6, (('P', 1, 4),)),
    ('oz', 5),
    (2, (('R', 1, 2),)),
    (3, (('P', 1, 0), ('R', 0, 3))),
    (4, (('P', 1, 4),)),
    (5, (('P', 0, 5),)),
    (6, (('R', 1, 3),)),
    (7, (('P', 0, 5), ('R', 0, 4))),
    ('g', 3),
    ('zf', 2),
    (0, (('P', 1, 5), ('Py+', 0, 7))),
    (2, (('P', 0, 4), ('P', 0, 1))),
    (3, (('P', 1, 3), ('P', 1, 1))),
    (7, (('P', 0, 0),)),
    ('g', 'V'),
    (0, (('R', 1, 1),)),
    (1, (('R', 0, 1), ('P', 0, 4))),
    (3, (('R', 0, 4),)),
    (5, (('P', 0, 6),)),
    (6, (('P', 1, 6), ('R', 1, 5), ('P', 1, 0))),
    (7, (('P', 0, 6),)),
    ('o', 0),
    (4, (('P', 1, 7),)),
    ('f', 3),
    (0, (('P', 1, 2),)),
    (2, (('R', 1, 3),)),
    ('zf', 0),
    ('f', 'V'),
    (2, (('P', 0, 5),)),
    ('o', 1),
    (0, (('P', 1, 7),)),
    (1, (('P', 0, 5),)),
    (2, (('P', 1, 6),)),
    (3, (('P', 0, 6),)),
    (6, (('P', 1, 2),)),
    ('z', 3),
    ('ou', 5),
    (7, (('P', 0, 3), ('P', 1, 4))),
    ('zf', 'V'),
    (5, (('P', 0, 7),)),
    (6, (('P', 0, 5),)),
    (7, (('P', 0, 7),)),
    ('oz', 6),
    ('zf', 1),
    (1, (('R', 0, 2),)),
    ('g', 4),
    (4, (('P', 1, 1),)),
    (5, (('P', 0, 1), ('P', 1, 0))),
    ('f', 4),
    (1, (('P', 0, 6),)),
    (2, (('P', 1, 1),)),
    (3, (('P', 0, 7),)),
    (4, (('P', 0, 0),)),
    (6, (('P', 0, 0),)),
    (7, (('P', 0, 4),)),
    ('oz', 7),
    ('zo', 0),
    (6, (('P', 0, 6), ('P', 1, 3))),
    ('o', 2),
    (2, (('P', 0, 2),)),
    (3, (('P', 0, 1),)),
    (7, (('P', 1, 7),)),
    ('ou', 6),
    (2, (('R', 1, 5),)),
    ('zg', 0),
    ('z', 5),
    (5, (('P', 0, 2),)),
    (7, (('P', 1, 0),)),
    ('z', 4),
    (2, (('P', 0, 6),)),
    (3, (('P', 1, 6), ('P', 1, 4))),
    ('zf', 3),
    (1, (('P', 0, 7),)),
    (4, (('P', 0, 3),)),
    (6, (('P', 0, 3),)),
    ('done', 0),
    (6, (('P', 1, 5),)),
    (7, (('P', 1, 6),)),
    ('zg', 1),
    ('f', 5),
    (2, (('P', 1, 7),)),
    (4, (('P', 0, 1),)),
    (5, (('P', 1, 2), ('P', 1, 1))),
    ('z', 6),
    (6, (('P', 0, 7),)),
    ('o', 'V'),
    ('g', 5),
    (3, (('P', 0, 2), ('P', 1, 5))),
    ('zo', 1),
    ('zg', 'V'),
    (6, (('P', 0, 4),)),
    (7, (('P', 1, 2),)),
    ('zo', 'V'),
    ('zo', 2),
    (6, (('P', 0, 1),)),
    ('ou', 7),
    (5, (('P', 1, 3),)),
    (6, (('P', 0, 2),)),
    (7, (('P', 1, 1),)),
    ('done', 1),
    ('z', 7),
    ('done', 'V'),
    ('done', 2),
    (4, (('P', 0, 4),)),
    (5, (('P', 0, 0),)),
    ('o', 3),
    ('zg', 3),
    (0, (('P', 1, 6),)),
    (2, (('P', 0, 7),)),
    (3, (('P', 1, 7),)),
    (4, (('P', 0, 2), ('P', 1, 0))),
    (7, (('P', 1, 3),)),
    ('o', 4),
    (5, (('P', 1, 5),)),
    ('zf', 5),
    (5, (('P', 0, 3),)),
    (6, (('P', 1, 7),)),
    (7, (('P', 0, 1),)),
    ('zg', 5),
    ('f', 6),
    ('zo', 3),
    ('zf', 4),
    (4, (('P', 1, 6),)),
    (7, (('P', 1, 5),)),
    ('zg', 4),
    (4, (('P', 1, 3),)),
    (5, (('P', 0, 4),)),
    (6, (('P', 1, 1),)),
    ('done', 3),
    ('o', 5),
    ('g', 6),
    ('f', 7),
    ('zg', 6),
    (7, (('P', 0, 2),)),
    ('S', 0),
    (2, (('P', 1, 4),)),
    (4, (('P', 1, 2),)),
    ('zf', 6),
    ('A', 0),
    ('g', 7),
    ('A', 1),
    ('A', 2),
    (4, (('P', 1, 5),)),
    ('zo', 5),
    ('o', 7),
    ('zf', 7),
    ('zg', 7),
    ('S', 1),
    ('zo', 4),
    ('o', 6),
    ('A', 3),
    ('done', 5),
    ('A', 5),
    ('zo', 6),
    ('B', 0),
    ('B', 1),
    ('zo', 7),
    ('B', 2),
    ('done', 6),
    ('B', 3),
    ('B', 5),
    ('done', 7),
    ('done', 4),
)
ROUTE = {
    (0, 0): (3, {0: {0: ['y+', 'y-'], 3: ['y-']}, 1: {3: ['y+', 'y-'], 0: ['y+']}}),
    (0, 1): (1, {0: {0: ['y+'], 1: ['y+'], 2: ['y+']}, 1: {1: ['y+', 'y-'], 0: ['y-']}}),
    (0, 2): (1, {0: {0: ['y+'], 1: ['y+'], 2: ['y+']}, 1: {1: ['y+', 'y-'], 0: ['y-']}}),
    (0, 3): (3, {0: {0: ['y+', 'y-'], 3: ['y-']}, 1: {3: ['y+', 'y-'], 0: ['y+']}}),
    (0, 4): (3, {0: {0: ['y+', 'y-'], 3: ['y-']}, 1: {3: ['y+', 'y-'], 2: ['y-']}}),
    (0, 5): (0, {0: {0: ['y+', 'y-'], 3: ['y-']}, 1: {0: ['y+', 'y-'], 1: ['y+']}}),
    (0, 6): (0, {0: {0: ['y+', 'y-'], 3: ['y-']}, 1: {0: ['y+', 'y-'], 1: ['y+']}}),
    (0, 7): (0, {0: {0: ['y+', 'y-'], 1: ['y+']}, 1: {0: ['y+', 'y-'], 1: ['y+']}}),
    (1, 0): (2, {0: {1: ['y+', 'y-'], 2: ['y+']}, 1: {2: ['y+', 'y-'], 3: ['y+']}}),
    (1, 1): (0, {0: {1: ['y-'], 0: ['y-'], 3: ['y-']}, 1: {0: ['y+', 'y-'], 3: ['y-']}}),
    (1, 2): (2, {0: {1: ['y+'], 2: ['y+'], 3: ['y+']}, 1: {2: ['y+', 'y-'], 3: ['y+']}}),
    (1, 3): (2, {0: {1: ['y+', 'y-'], 2: ['y+']}, 1: {2: ['y+', 'y-'], 1: ['y-']}}),
    (1, 4): (1, {0: {1: ['y-'], 0: ['y-'], 3: ['y-']}, 1: {1: ['y+', 'y-'], 2: ['y+']}}),
    (1, 5): (2, {0: {1: ['y+', 'y-'], 0: ['y-']}, 1: {2: ['y+', 'y-'], 1: ['y-']}}),
    (1, 6): (1, {0: {1: ['y+'], 2: ['y+'], 3: ['y+']}, 1: {1: ['y+'], 2: ['y+'], 3: ['y+']}}),
    (1, 7): (1, {0: {1: ['y+', 'y-'], 2: ['y+']}, 1: {1: ['y-'], 0: ['y-'], 3: ['y-']}}),
}
CHUNKS = ((0, 640), (640, 640), (1280, 640), (1920, 640), (2560, 640), (3200, 640), (3840, 640), (4480, 520))
TAIL = (4, 6, 7)
Z, M, PL, O, ZM, ZP, ZO = range(7)


def kernel(m_hbm, l_hbm, d_hbm, out, solved, lbuf, pbuf, rbuf, vbuf, dbuf, acc,
           load_sem, l_recv, l_sib, l_send, v_recv, v_send, p_recv, r_recv, p_send, ready_sem):
    aux, pair = lax.axis_index("aux"), lax.axis_index("pair")
    zh, y = aux // 4, aux % 4
    zl, x, c = pair // 8, (pair // 2) % 4, pair % 2
    nb = l_hbm.shape[1]
    nrows = l_hbm.shape[2]
    nk = nb * 16
    nchunk = len(TYPES)
    piece = nk // NP
    half = piece // 2
    f32, bf16 = jnp.float32, jnp.bfloat16

    def at_pair(xx, zz, cc):
        return zz * 8 + lax.rem(xx + 8, 4) * 2 + cc

    sib = (aux, at_pair(x, zl, 1 - c))
    dev = {
        "x+": (aux, at_pair(x + 1, zl, c)),
        "x-": (aux, at_pair(x - 1, zl, c)),
        "y+": (zh * 4 + lax.rem(y + 1, 4), pair),
        "y-": (zh * 4 + lax.rem(y + 3, 4), pair),
        "zi": (aux, at_pair(x, 1 - zl, c)),
        "zo": ((1 - zh) * 4 + y, at_pair(x, 1 - zl, c)),
        "sib": sib,
    }

    own = pl.ds(pl.multiple_of(pair * nb, nb), nb)
    load_l = pltpu.make_async_copy(l_hbm, lbuf.at[:, own, :], load_sem.at[0])
    load_l.start()
    load_d = pltpu.make_async_copy(d_hbm, dbuf, load_sem.at[1])
    load_d.start()
    is_src = [aux == q for q in range(2)]
    load_p = [pltpu.make_async_copy(m_hbm.at[pl.ds(0, nk), :], pbuf.at[q], load_sem.at[2]) for q in range(2)]
    load_v = pltpu.make_async_copy(l_hbm.at[0, :, pl.ds(0, nk)], vbuf.at[own, :], load_sem.at[3])
    for q in range(2):
        pl.when(is_src[q])(load_p[q].start)
    pl.when(is_src[1])(load_v.start)
    load_m = pltpu.make_async_copy(m_hbm, out, load_sem.at[4])
    load_m.start()

    barrier = pltpu.get_barrier_semaphore()
    for d in dev.values():
        pl.semaphore_signal(barrier, inc=1, device_id=d, device_id_type=MESH)
    for k in range(1, 8):
        @pl.when(is_src[1])
        def _(k=k):
            pl.semaphore_signal(barrier, inc=1, device_id=(lax.rem(aux + k, 8), pair), device_id_type=MESH)

    @pl.when(jnp.logical_not(is_src[1]))
    def _():
        pl.semaphore_wait(barrier, 8)
        pl.semaphore_signal(ready_sem, inc=1, device_id=(1, pair), device_id_type=MESH)

    @pl.when(is_src[1])
    def _():
        pl.semaphore_wait(barrier, 7)

    def rows_of(r):
        return pl.ds(*CHUNKS[r])

    def slot(r, first, count=nb):
        if r == "V":
            return vbuf.at[pl.ds(first, count), :]
        return lbuf.at[:, pl.ds(first, count), rows_of(r)]

    def index(r):
        return nchunk if r == "V" else r

    def kind(r):
        return "A" if r == "V" else TYPES[r]

    def parity(r):
        return 0 if r == "V" else TYPES[:r].count("B") % 2

    def message(r, xx, zz, to, sem):
        ref = slot(r, pl.multiple_of(at_pair(xx, zz, c) * nb, nb))
        return pltpu.make_async_remote_copy(ref, ref, l_send.at[index(r)], sem, device_id=to, device_id_type=MESH)

    def send(r, xx, zz, to, name):
        message(r, xx, zz, to, l_recv.at[index(r), name]).start()

    def sibling(r, xx, zz):
        message(r, xx, zz, sib, l_sib.at[index(r)]).start()

    def wait(r, xx, zz, name):
        message(r, xx, zz, sib, l_recv.at[index(r), name]).wait_recv()

    def sign(r, z_dyn):
        return z_dyn if kind(r) == "A" else lax.rem(z_dyn + parity(r), 2)

    def ev_oz(r):
        if r == "V":
            pl.when(jnp.logical_not(is_src[1]))(v_copy(1).wait_recv)
            ev_ou(r)
            ev_od(r)
        send(r, x, zl, dev["zi"], Z)

    def ev_ou(r):
        send(r, x, zl, dev["x+"], M)

    def ev_od(r):
        send(r, x, zl, dev["x-"], PL)
        sibling(r, x, zl)

    def across(r, xx, name):
        if kind(r) == "B":
            send(r, xx, zl, dev["zi"], name)

    def ev_f(r):
        s = sign(r, zl)
        step = 1 - 2 * s
        wait(r, x - step, zl, M + s)
        send(r, x - step, zl, (aux, at_pair(x + step, zl, c)), O)
        sibling(r, x - step, zl)
        across(r, x - step, ZM + s)

    def ev_g(r):
        s = sign(r, zl)
        step = 1 - 2 * s
        wait(r, x + step, zl, PL - s)
        sibling(r, x + step, zl)
        across(r, x + step, ZP - s)

    def ev_o(r):
        wait(r, x + 2, zl, O)
        sibling(r, x + 2, zl)
        across(r, x + 2, ZO)

    def ev_z(r):
        wait(r, x, 1 - zl, Z)
        if kind(r) == "A":
            send(r, x, 1 - zl, dev["x+"], ZM)
            send(r, x, 1 - zl, dev["x-"], ZP)
        sibling(r, x, 1 - zl)

    def ev_zf(r):
        s = sign(r, 1 - zl)
        step = 1 - 2 * s
        wait(r, x - step, 1 - zl, ZM + s)
        if kind(r) == "A":
            send(r, x - step, 1 - zl, (aux, at_pair(x + step, zl, c)), ZO)
        sibling(r, x - step, 1 - zl)

    def ev_zg(r):
        s = sign(r, 1 - zl)
        step = 1 - 2 * s
        wait(r, x + step, 1 - zl, ZP - s)
        sibling(r, x + step, 1 - zl)

    def ev_zo(r):
        wait(r, x + 2, 1 - zl, ZO)
        sibling(r, x + 2, 1 - zl)

    def ev_done(r):
        pltpu.make_async_remote_copy(slot(r, 0, 8 * nb), slot(r, 0, 8 * nb), l_send.at[index(r)], l_sib.at[index(r)],
                                     device_id=sib, device_id_type=MESH).wait_recv()

    def ev_sent(r):
        pltpu.make_async_remote_copy(slot(r, 0, 15 * nb), slot(r, 0, 15 * nb), l_send.at[index(r)], l_sib.at[index(r)],
                                     device_id=sib, device_id_type=MESH).wait_send()

    LINKS = ("y+", "y-", "zo", "zi")
    sent = {a: [] for a in range(8)}

    def p_copy(q, i, k, src, dst, to, sem):
        return pltpu.make_async_remote_copy(src, dst, p_send.at[q, i, k], sem, device_id=dev[to], device_id_type=MESH)

    def pivot(a, name, q, i):
        a_zh, a_y = a // 4, a % 4
        cross, trees = ROUTE[q, i]
        full = pbuf.at[q, pl.ds(i * piece, piece), :]
        first = pbuf.at[q, pl.ds(i * piece, half), :]
        second = pbuf.at[q, pl.ds(i * piece + half, half), :]
        relay = rbuf.at[q, pl.ds(i * half, half), :]
        got, rel = p_recv.at[q, i], r_recv.at[q, i]

        def go(k, src, dst, to, sem):
            copy = p_copy(q, i, k, src, dst, to, sem)
            copy.start()
            sent[a].append((q, i, k, src is full))

        if name == "P":
            p_copy(q, i, 0, full, full, "y+", got).wait_recv()
        if name == "X" or (name == "P" and a_zh == 0 and a_y == cross):
            go(2, second, relay, "zo", rel)
            go(3, first, relay, "zi", rel)
        if name[0] == "P":
            for link in trees[a_zh].get(a_y, ()):
                if name in ("P", "P" + link):
                    go(LINKS.index(link), full, full, link, got)
        if name == "R":
            p_copy(q, i, 4, relay, relay, "zi", rel).wait_recv()
            if a_zh == 0:
                go(4, relay, first, "zo", got)
            else:
                go(4, relay, second, "zi", got)

    def v_copy(k):
        ref = vbuf.at[own, :]
        return pltpu.make_async_remote_copy(ref, ref, v_send.at[k], v_recv.at[0], device_id=(lax.rem(aux + k, 8), pair), device_id_type=MESH)

    def ev_v():
        @pl.when(is_src[1])
        def _():
            load_v.wait()
            pl.semaphore_wait(ready_sem, 7)
            for k in range(1, 8):
                v_copy(k).start()

    def halves(v):
        h = v.astype(bf16)
        return h, (v - h.astype(f32)).astype(bf16)

    def dot(a, b):
        return jnp.dot(a, b, preferred_element_type=f32)

    def dot_t(a, b):
        return lax.dot_general(a, b, (((0,), (0,)), ((), ())), preferred_element_type=f32)

    width = 256
    cols = [pl.ds(n * width, width) for n in range(out.shape[1] // width)]

    def solve(q):
        dh, dl = halves(dbuf[q])
        for n in cols:
            if q == 0:
                p = pbuf[0, :, n]
                s = dot(dh, p) + dot(dl, p)
            else:
                w = pbuf[1, :, n].astype(f32) - dot_t(vbuf[...], solved[0, :, n])
                wh, wl = halves(w)
                s = dot(dh, wh) + dot(dl, wh) + dot(dh, wl)
            solved[q, :, n] = s.astype(bf16)

    def product(rows, q, last):
        lq = [lbuf[k, :, rows] for k in range(q, last + 1)]
        for n in cols:
            o = out[rows, n].astype(f32) if q == 0 else acc[rows, n]
            for k in range(q, last + 1):
                o = o - dot_t(lq[k - q], solved[k, :, n])
            if last == 1:
                out[rows, n] = o.astype(bf16)
            else:
                acc[rows, n] = o

    load_l.wait()
    for q in range(2):
        pl.when(is_src[q])(load_p[q].wait)
    act = {"oz": ev_oz, "ou": ev_ou, "od": ev_od, "z": ev_z, "f": ev_f, "g": ev_g, "o": ev_o,
           "zf": ev_zf, "zg": ev_zg, "zo": ev_zo, "done": ev_done}
    chunks = ["V"] + list(range(nchunk))
    skip = False
    for n, step in enumerate(ORDER):
        if n == 15:
            ev_v()
        name, r = step
        if name in act:
            act[name](r)
        elif name == "S":
            if r == 0:
                load_d.wait()
                load_m.wait()
            solve(r)
        elif name == "A":
            skip = ("B", r) == (ORDER + ((),))[n + 1]
            product(rows_of(r), 0, 1 if skip else 0)
        elif name == "B":
            if not skip:
                product(rows_of(r), 1, 1)
            skip = False
        else:
            @pl.when(aux == name)
            def _(a=name, todo=r):
                for what, q, i in todo:
                    pivot(a, what, q, i)

    for r in chunks:
        ev_sent(r)
    for a in sent:
        @pl.when(aux == a)
        def _(a=a):
            for q, i, k, whole in sent[a]:
                ref = pbuf.at[q, pl.ds(i * piece, piece if whole else half), :]
                p_copy(q, i, k, ref, ref, "y+", p_recv.at[q, i]).wait_send()

    @pl.when(is_src[1])
    def _():
        for k in range(1, 8):
            v_copy(k).wait_send()


def finish(part, lbuf, solved, out_hbm, solved_hbm, late, sems):
    f32, bf16 = jnp.float32, jnp.bfloat16
    n_sem = iter(range(2 + len(CHUNKS)))
    copies = [pltpu.make_async_copy(solved, solved_hbm, sems.at[next(n_sem)])]
    ready = sorted(CHUNKS[r] for r in range(len(CHUNKS)) if r not in TAIL)
    runs = []
    for start, size in ready:
        if runs and runs[-1][0] + runs[-1][1] == start:
            runs[-1][1] += size
        else:
            runs.append([start, size])
    for start, size in runs:
        rows = pl.ds(start, size)
        copies.append(pltpu.make_async_copy(part.at[rows, :], out_hbm.at[rows, :], sems.at[next(n_sem)]))
    for copy in copies:
        copy.start()
    base = 0
    width = 256
    for r in TAIL:
        start, size = CHUNKS[r]
        rows = pl.ds(start, size)
        lq = [lbuf[k, :, rows] for k in range(2)]
        for c in range(part.shape[1] // width):
            n = pl.ds(c * width, width)
            o = part[rows, n].astype(f32)
            for k in range(2):
                o = o - lax.dot_general(lq[k], solved[k, :, n], (((0,), (0,)), ((), ())), preferred_element_type=f32)
            late[pl.ds(base, size), n] = o.astype(bf16)
        copy = pltpu.make_async_copy(late.at[pl.ds(base, size), :], out_hbm.at[rows, :], sems.at[next(n_sem)])
        copy.start()
        copies.append(copy)
        base += size
    for copy in copies:
        copy.wait()


def solution(mesh):
    def step(m_panels, lower_cols, diag_inverses):
        rows, cols = m_panels.shape
        panels, nk, _ = diag_inverses.shape
        dma = pltpu.SemaphoreType.DMA
        n = len(TYPES) + 1
        bf16 = jnp.bfloat16
        part, solved, lbuf = pl.pallas_call(
            kernel,
            out_shape=(
                pltpu.VMEM((rows, cols), bf16),
                pltpu.VMEM((panels, nk, cols), bf16),
                pltpu.VMEM((panels, nk, rows), bf16),
            ),
            in_specs=[pl.BlockSpec(memory_space=pltpu.HBM)] * 3,
            out_specs=(pl.BlockSpec(memory_space=pltpu.VMEM),) * 3,
            scratch_shapes=[
                pltpu.VMEM((panels, nk, cols), bf16),
                pltpu.VMEM((panels, nk // 2, cols), bf16),
                pltpu.VMEM((nk, nk), bf16),
                pltpu.VMEM((panels, nk, nk), jnp.float32),
                pltpu.VMEM((rows, cols), jnp.float32),
                dma((5,)), dma((n, 7)), dma((n,)), dma((n,)), dma((1,)), dma((8,)),
                dma((panels, NP)), dma((panels, NP)), dma((panels, NP, 5)), pltpu.SemaphoreType.REGULAR,
            ],
            compiler_params=pltpu.CompilerParams(collective_id=0, has_side_effects=True, vmem_limit_bytes=36 * 2**20),
        )(m_panels, lower_cols, diag_inverses)
        late = -(-sum(CHUNKS[r][1] for r in TAIL) // 16) * 16
        return pl.pallas_call(
            finish,
            out_shape=(jax.ShapeDtypeStruct((rows, cols), bf16), jax.ShapeDtypeStruct((panels, nk, cols), bf16)),
            in_specs=[pl.BlockSpec(memory_space=pltpu.VMEM)] * 3,
            out_specs=(pl.BlockSpec(memory_space=pltpu.HBM),) * 2,
            scratch_shapes=[pltpu.VMEM((late, cols), bf16), dma((2 + len(CHUNKS),))],
            compiler_params=pltpu.CompilerParams(vmem_limit_bytes=12 * 2**20),
        )(*(pltpu.with_memory_space_constraint(v, pltpu.VMEM) for v in (part, lbuf, solved)))

    return jax.shard_map(
        step,
        mesh=mesh,
        in_specs=(P("aux", "pair"), P(None, "pair", "aux"), P()),
        out_specs=(P("aux", "pair"), P(None, None, "pair")),
        check_vma=False,
    )
```

```python
import functools

import jax
import jax.numpy as jnp
from jax import lax
from jax.experimental import pallas as pl
from jax.experimental.pallas import tpu as pltpu
from jax.sharding import PartitionSpec as P

MESH = pl.DeviceIdType.MESH
TYPES = "AABAABAA"
NP = 8
ORDER = (
    ('ou', 0),
    (0, (('X', 0, 6), ('Py+', 0, 0), ('Py+', 0, 1), ('Py-', 0, 0), ('Py-', 0, 3))),
    (1, (('Py-', 1, 0), ('Py+', 1, 0), ('Py+', 1, 2), ('Py-', 1, 1), ('X', 1, 4), ('X', 1, 6), ('X', 1, 7))),
    ('od', 0),
    ('od', 1),
    ('od', 2),
    ('od', 4),
    ('od', 5),
    ('od', 6),
    ('od', 7),
    ('ou', 1),
    (0, (('X', 0, 5),)),
    ('ou', 2),
    (0, (('X', 0, 7),)),
    ('oz', 1),
    ('oz', 0),
    ('od', 3),
    ('oz', 2),
    (0, (('Py+', 0, 2), ('Py-', 0, 4), ('R', 0, 5))),
    (1, (('Py-', 1, 3), ('Py+', 1, 3), ('Py+', 1, 5), ('R', 1, 4))),
    (4, (('R', 0, 5),)),
    (5, (('R', 1, 4),)),
    ('g', 0),
    ('f', 0),
    (0, (('P', 1, 0), ('R', 0, 6), ('Py+', 0, 3), ('Py-', 0, 5))),
    (1, (('P', 0, 0), ('R', 1, 6), ('Py-', 1, 4))),
    (2, (('P', 1, 0),)),
    (3, (('P', 0, 0),)),
    (4, (('R', 0, 6),)),
    (5, (('R', 1, 6),)),
    ('f', 1),
    (0, (('R', 0, 7),)),
    (1, (('R', 1, 7),)),
    (4, (('R', 0, 7),)),
    (5, (('R', 1, 7), ('P', 1, 4))),
    ('oz', 'V'),
    ('g', 2),
    ('f', 2),
    (0, (('P', 1, 1),)),
    (1, (('P', 0, 1),)),
    (2, (('P', 1, 2),)),
    (3, (('P', 0, 3),)),
    ('oz', 3),
    (0, (('Py+', 0, 4),)),
    (1, (('Py+', 1, 6), ('Py-', 1, 5))),
    ('g', 1),
    (4, (('P', 0, 5),)),
    (6, (('R', 1, 0),)),
    (7, (('R', 0, 0),)),
    ('z', 0),
    (0, (('Py-', 0, 6),)),
    (2, (('R', 1, 0),)),
    ('ou', 3),
    ('z', 1),
    (0, (('Py+', 0, 5), ('P', 1, 3), ('Py-', 0, 7))),
    (1, (('P', 0, 2), ('Py+', 1, 7), ('Py-', 1, 7))),
    (2, (('P', 0, 0), ('P', 1, 3))),
    (3, (('P', 0, 4),)),
    (4, (('P', 0, 6),)),
    (5, (('P', 1, 6),)),
    ('ou', 4),
    ('z', 2),
    (3, (('R', 0, 0),)),
    (4, (('R', 1, 1), ('P', 0, 7))),
    (5, (('R', 0, 1),)),
    (6, (('R', 1, 2),)),
    (7, (('R', 0, 3),)),
    ('z', 'V'),
    (5, (('P', 1, 7), ('R', 0, 2))),
    ('zg', 2),
    (2, (('P', 0, 3),)),
    (3, (('P', 1, 2),)),
    ('oz', 4),
    (0, (('P', 1, 4), ('Py+', 0, 6))),
    (1, (('P', 0, 3),)),
    (2, (('P', 1, 5),)),
    (3, (('P', 0, 5),)),
    (6, (('P', 1, 4),)),
    ('oz', 5),
    (2, (('R', 1, 2),)),
    (3, (('P', 1, 0), ('R', 0, 3))),
    (4, (('P', 1, 4),)),
    (5, (('P', 0, 5),)),
    (6, (('R', 1, 3),)),
    (7, (('P', 0, 5), ('R', 0, 4))),
    ('g', 3),
    ('zf', 2),
    (0, (('P', 1, 5), ('Py+', 0, 7))),
    (2, (('P', 0, 4), ('P', 0, 1))),
    (3, (('P', 1, 3), ('P', 1, 1))),
    (7, (('P', 0, 0),)),
    ('g', 'V'),
    (0, (('R', 1, 1),)),
    (1, (('R', 0, 1), ('P', 0, 4))),
    (3, (('R', 0, 4),)),
    (5, (('P', 0, 6),)),
    (6, (('P', 1, 6), ('R', 1, 5), ('P', 1, 0))),
    (7, (('P', 0, 6),)),
    ('o', 0),
    (4, (('P', 1, 7),)),
    ('f', 3),
    (0, (('P', 1, 2),)),
    (2, (('R', 1, 3),)),
    ('zf', 0),
    ('f', 'V'),
    (2, (('P', 0, 5),)),
    ('o', 1),
    (0, (('P', 1, 7),)),
    (1, (('P', 0, 5),)),
    (2, (('P', 1, 6),)),
    (3, (('P', 0, 6),)),
    (6, (('P', 1, 2),)),
    ('z', 3),
    ('ou', 5),
    (7, (('P', 0, 3), ('P', 1, 4))),
    ('zf', 'V'),
    (5, (('P', 0, 7),)),
    (6, (('P', 0, 5),)),
    (7, (('P', 0, 7),)),
    ('oz', 6),
    ('zf', 1),
    (1, (('R', 0, 2),)),
    ('g', 4),
    (4, (('P', 1, 1),)),
    (5, (('P', 0, 1), ('P', 1, 0))),
    ('f', 4),
    (1, (('P', 0, 6),)),
    (2, (('P', 1, 1),)),
    (3, (('P', 0, 7),)),
    (4, (('P', 0, 0),)),
    (6, (('P', 0, 0),)),
    (7, (('P', 0, 4),)),
    ('oz', 7),
    ('zo', 0),
    (6, (('P', 0, 6), ('P', 1, 3))),
    ('o', 2),
    (2, (('P', 0, 2),)),
    (3, (('P', 0, 1),)),
    (7, (('P', 1, 7),)),
    ('ou', 6),
    (2, (('R', 1, 5),)),
    ('zg', 0),
    ('z', 5),
    (5, (('P', 0, 2),)),
    (7, (('P', 1, 0),)),
    ('z', 4),
    (2, (('P', 0, 6),)),
    (3, (('P', 1, 6), ('P', 1, 4))),
    ('zf', 3),
    (1, (('P', 0, 7),)),
    (4, (('P', 0, 3),)),
    (6, (('P', 0, 3),)),
    ('done', 0),
    (6, (('P', 1, 5),)),
    (7, (('P', 1, 6),)),
    ('zg', 1),
    ('f', 5),
    (2, (('P', 1, 7),)),
    (4, (('P', 0, 1),)),
    (5, (('P', 1, 2), ('P', 1, 1))),
    ('z', 6),
    (6, (('P', 0, 7),)),
    ('o', 'V'),
    ('g', 5),
    (3, (('P', 0, 2), ('P', 1, 5))),
    ('zo', 1),
    ('zg', 'V'),
    (6, (('P', 0, 4),)),
    (7, (('P', 1, 2),)),
    ('zo', 'V'),
    ('zo', 2),
    (6, (('P', 0, 1),)),
    ('ou', 7),
    (5, (('P', 1, 3),)),
    (6, (('P', 0, 2),)),
    (7, (('P', 1, 1),)),
    ('done', 1),
    ('z', 7),
    ('done', 'V'),
    ('done', 2),
    (4, (('P', 0, 4),)),
    (5, (('P', 0, 0),)),
    ('o', 3),
    ('zg', 3),
    (0, (('P', 1, 6),)),
    (2, (('P', 0, 7),)),
    (3, (('P', 1, 7),)),
    (4, (('P', 0, 2), ('P', 1, 0))),
    (7, (('P', 1, 3),)),
    ('o', 4),
    (5, (('P', 1, 5),)),
    ('zf', 5),
    (5, (('P', 0, 3),)),
    (6, (('P', 1, 7),)),
    (7, (('P', 0, 1),)),
    ('zg', 5),
    ('f', 6),
    ('zo', 3),
    ('zf', 4),
    (4, (('P', 1, 6),)),
    (7, (('P', 1, 5),)),
    ('zg', 4),
    (4, (('P', 1, 3),)),
    (5, (('P', 0, 4),)),
    (6, (('P', 1, 1),)),
    ('done', 3),
    ('o', 5),
    ('g', 6),
    ('f', 7),
    ('zg', 6),
    (7, (('P', 0, 2),)),
    ('S', 0),
    (2, (('P', 1, 4),)),
    (4, (('P', 1, 2),)),
    ('zf', 6),
    ('A', 0),
    ('g', 7),
    ('A', 1),
    ('A', 2),
    (4, (('P', 1, 5),)),
    ('zo', 5),
    ('o', 7),
    ('zf', 7),
    ('zg', 7),
    ('S', 1),
    ('zo', 4),
    ('o', 6),
    ('A', 3),
    ('done', 5),
    ('A', 5),
    ('zo', 6),
    ('B', 0),
    ('B', 1),
    ('zo', 7),
    ('B', 2),
    ('done', 6),
    ('B', 3),
    ('B', 5),
    ('done', 7),
    ('done', 4),
)
ROUTE = {
    (0, 0): (3, {0: {0: ['y+', 'y-'], 3: ['y-']}, 1: {3: ['y+', 'y-'], 0: ['y+']}}),
    (0, 1): (1, {0: {0: ['y+'], 1: ['y+'], 2: ['y+']}, 1: {1: ['y+', 'y-'], 0: ['y-']}}),
    (0, 2): (1, {0: {0: ['y+'], 1: ['y+'], 2: ['y+']}, 1: {1: ['y+', 'y-'], 0: ['y-']}}),
    (0, 3): (3, {0: {0: ['y+', 'y-'], 3: ['y-']}, 1: {3: ['y+', 'y-'], 0: ['y+']}}),
    (0, 4): (3, {0: {0: ['y+', 'y-'], 3: ['y-']}, 1: {3: ['y+', 'y-'], 2: ['y-']}}),
    (0, 5): (0, {0: {0: ['y+', 'y-'], 3: ['y-']}, 1: {0: ['y+', 'y-'], 1: ['y+']}}),
    (0, 6): (0, {0: {0: ['y+', 'y-'], 3: ['y-']}, 1: {0: ['y+', 'y-'], 1: ['y+']}}),
    (0, 7): (0, {0: {0: ['y+', 'y-'], 1: ['y+']}, 1: {0: ['y+', 'y-'], 1: ['y+']}}),
    (1, 0): (2, {0: {1: ['y+', 'y-'], 2: ['y+']}, 1: {2: ['y+', 'y-'], 3: ['y+']}}),
    (1, 1): (0, {0: {1: ['y-'], 0: ['y-'], 3: ['y-']}, 1: {0: ['y+', 'y-'], 3: ['y-']}}),
    (1, 2): (2, {0: {1: ['y+'], 2: ['y+'], 3: ['y+']}, 1: {2: ['y+', 'y-'], 3: ['y+']}}),
    (1, 3): (2, {0: {1: ['y+', 'y-'], 2: ['y+']}, 1: {2: ['y+', 'y-'], 1: ['y-']}}),
    (1, 4): (1, {0: {1: ['y-'], 0: ['y-'], 3: ['y-']}, 1: {1: ['y+', 'y-'], 2: ['y+']}}),
    (1, 5): (2, {0: {1: ['y+', 'y-'], 0: ['y-']}, 1: {2: ['y+', 'y-'], 1: ['y-']}}),
    (1, 6): (1, {0: {1: ['y+'], 2: ['y+'], 3: ['y+']}, 1: {1: ['y+'], 2: ['y+'], 3: ['y+']}}),
    (1, 7): (1, {0: {1: ['y+', 'y-'], 2: ['y+']}, 1: {1: ['y-'], 0: ['y-'], 3: ['y-']}}),
}
CHUNKS = ((0, 640), (640, 640), (1280, 640), (1920, 640), (2560, 640), (3200, 640), (3840, 640), (4480, 520))
TAIL = (4, 6, 7)
Z, M, PL, O, ZM, ZP, ZO = range(7)


def kernel(m_hbm, l_hbm, d_hbm, out, solved, lbuf, pbuf, rbuf, vbuf, dbuf, acc,
           load_sem, l_recv, l_sib, l_send, v_recv, v_send, p_recv, r_recv, p_send, ready_sem):
    aux, pair = lax.axis_index("aux"), lax.axis_index("pair")
    zh, y = aux // 4, aux % 4
    zl, x, c = pair // 8, (pair // 2) % 4, pair % 2
    nb = l_hbm.shape[1]
    nrows = l_hbm.shape[2]
    nk = nb * 16
    nchunk = len(TYPES)
    piece = nk // NP
    half = piece // 2
    f32, bf16 = jnp.float32, jnp.bfloat16

    def at_pair(xx, zz, cc):
        return zz * 8 + lax.rem(xx + 8, 4) * 2 + cc

    sib = (aux, at_pair(x, zl, 1 - c))
    dev = {
        "x+": (aux, at_pair(x + 1, zl, c)),
        "x-": (aux, at_pair(x - 1, zl, c)),
        "y+": (zh * 4 + lax.rem(y + 1, 4), pair),
        "y-": (zh * 4 + lax.rem(y + 3, 4), pair),
        "zi": (aux, at_pair(x, 1 - zl, c)),
        "zo": ((1 - zh) * 4 + y, at_pair(x, 1 - zl, c)),
        "sib": sib,
    }

    own = pl.ds(pl.multiple_of(pair * nb, nb), nb)
    load_l = pltpu.make_async_copy(l_hbm, lbuf.at[:, own, :], load_sem.at[0])
    load_l.start()
    load_d = pltpu.make_async_copy(d_hbm, dbuf, load_sem.at[1])
    load_d.start()
    is_src = [aux == q for q in range(2)]
    load_p = [pltpu.make_async_copy(m_hbm.at[pl.ds(0, nk), :], pbuf.at[q], load_sem.at[2]) for q in range(2)]
    load_v = pltpu.make_async_copy(l_hbm.at[0, :, pl.ds(0, nk)], vbuf.at[own, :], load_sem.at[3])
    for q in range(2):
        pl.when(is_src[q])(load_p[q].start)
    pl.when(is_src[1])(load_v.start)
    load_m = pltpu.make_async_copy(m_hbm, out, load_sem.at[4])
    load_m.start()

    barrier = pltpu.get_barrier_semaphore()
    for d in dev.values():
        pl.semaphore_signal(barrier, inc=1, device_id=d, device_id_type=MESH)
    for k in range(1, 8):
        @pl.when(is_src[1])
        def _(k=k):
            pl.semaphore_signal(barrier, inc=1, device_id=(lax.rem(aux + k, 8), pair), device_id_type=MESH)

    @pl.when(jnp.logical_not(is_src[1]))
    def _():
        pl.semaphore_wait(barrier, 8)
        pl.semaphore_signal(ready_sem, inc=1, device_id=(1, pair), device_id_type=MESH)

    @pl.when(is_src[1])
    def _():
        pl.semaphore_wait(barrier, 7)

    def rows_of(r):
        return pl.ds(*CHUNKS[r])

    def slot(r, first, count=nb):
        if r == "V":
            return vbuf.at[pl.ds(first, count), :]
        return lbuf.at[:, pl.ds(first, count), rows_of(r)]

    def index(r):
        return nchunk if r == "V" else r

    def kind(r):
        return "A" if r == "V" else TYPES[r]

    def parity(r):
        return 0 if r == "V" else TYPES[:r].count("B") % 2

    def message(r, xx, zz, to, sem):
        ref = slot(r, pl.multiple_of(at_pair(xx, zz, c) * nb, nb))
        return pltpu.make_async_remote_copy(ref, ref, l_send.at[index(r)], sem, device_id=to, device_id_type=MESH)

    def send(r, xx, zz, to, name):
        message(r, xx, zz, to, l_recv.at[index(r), name]).start()

    def sibling(r, xx, zz):
        message(r, xx, zz, sib, l_sib.at[index(r)]).start()

    def wait(r, xx, zz, name):
        message(r, xx, zz, sib, l_recv.at[index(r), name]).wait_recv()

    def sign(r, z_dyn):
        return z_dyn if kind(r) == "A" else lax.rem(z_dyn + parity(r), 2)

    def ev_oz(r):
        if r == "V":
            pl.when(jnp.logical_not(is_src[1]))(v_copy(1).wait_recv)
            ev_ou(r)
            ev_od(r)
        send(r, x, zl, dev["zi"], Z)

    def ev_ou(r):
        send(r, x, zl, dev["x+"], M)

    def ev_od(r):
        send(r, x, zl, dev["x-"], PL)
        sibling(r, x, zl)

    def across(r, xx, name):
        if kind(r) == "B":
            send(r, xx, zl, dev["zi"], name)

    def ev_f(r):
        s = sign(r, zl)
        step = 1 - 2 * s
        wait(r, x - step, zl, M + s)
        send(r, x - step, zl, (aux, at_pair(x + step, zl, c)), O)
        sibling(r, x - step, zl)
        across(r, x - step, ZM + s)

    def ev_g(r):
        s = sign(r, zl)
        step = 1 - 2 * s
        wait(r, x + step, zl, PL - s)
        sibling(r, x + step, zl)
        across(r, x + step, ZP - s)

    def ev_o(r):
        wait(r, x + 2, zl, O)
        sibling(r, x + 2, zl)
        across(r, x + 2, ZO)

    def ev_z(r):
        wait(r, x, 1 - zl, Z)
        if kind(r) == "A":
            send(r, x, 1 - zl, dev["x+"], ZM)
            send(r, x, 1 - zl, dev["x-"], ZP)
        sibling(r, x, 1 - zl)

    def ev_zf(r):
        s = sign(r, 1 - zl)
        step = 1 - 2 * s
        wait(r, x - step, 1 - zl, ZM + s)
        if kind(r) == "A":
            send(r, x - step, 1 - zl, (aux, at_pair(x + step, zl, c)), ZO)
        sibling(r, x - step, 1 - zl)

    def ev_zg(r):
        s = sign(r, 1 - zl)
        step = 1 - 2 * s
        wait(r, x + step, 1 - zl, ZP - s)
        sibling(r, x + step, 1 - zl)

    def ev_zo(r):
        wait(r, x + 2, 1 - zl, ZO)
        sibling(r, x + 2, 1 - zl)

    def ev_done(r):
        pltpu.make_async_remote_copy(slot(r, 0, 8 * nb), slot(r, 0, 8 * nb), l_send.at[index(r)], l_sib.at[index(r)],
                                     device_id=sib, device_id_type=MESH).wait_recv()

    def ev_sent(r):
        pltpu.make_async_remote_copy(slot(r, 0, 15 * nb), slot(r, 0, 15 * nb), l_send.at[index(r)], l_sib.at[index(r)],
                                     device_id=sib, device_id_type=MESH).wait_send()

    LINKS = ("y+", "y-", "zo", "zi")
    sent = {a: [] for a in range(8)}

    def p_copy(q, i, k, src, dst, to, sem):
        return pltpu.make_async_remote_copy(src, dst, p_send.at[q, i, k], sem, device_id=dev[to], device_id_type=MESH)

    def pivot(a, name, q, i):
        a_zh, a_y = a // 4, a % 4
        cross, trees = ROUTE[q, i]
        full = pbuf.at[q, pl.ds(i * piece, piece), :]
        first = pbuf.at[q, pl.ds(i * piece, half), :]
        second = pbuf.at[q, pl.ds(i * piece + half, half), :]
        relay = rbuf.at[q, pl.ds(i * half, half), :]
        got, rel = p_recv.at[q, i], r_recv.at[q, i]

        def go(k, src, dst, to, sem):
            copy = p_copy(q, i, k, src, dst, to, sem)
            copy.start()
            sent[a].append((q, i, k, src is full))

        if name == "P":
            p_copy(q, i, 0, full, full, "y+", got).wait_recv()
        if name == "X" or (name == "P" and a_zh == 0 and a_y == cross):
            go(2, second, relay, "zo", rel)
            go(3, first, relay, "zi", rel)
        if name[0] == "P":
            for link in trees[a_zh].get(a_y, ()):
                if name in ("P", "P" + link):
                    go(LINKS.index(link), full, full, link, got)
        if name == "R":
            p_copy(q, i, 4, relay, relay, "zi", rel).wait_recv()
            if a_zh == 0:
                go(4, relay, first, "zo", got)
            else:
                go(4, relay, second, "zi", got)

    def v_copy(k):
        ref = vbuf.at[own, :]
        return pltpu.make_async_remote_copy(ref, ref, v_send.at[k], v_recv.at[0], device_id=(lax.rem(aux + k, 8), pair), device_id_type=MESH)

    def ev_v():
        @pl.when(is_src[1])
        def _():
            load_v.wait()
            pl.semaphore_wait(ready_sem, 7)
            for k in range(1, 8):
                v_copy(k).start()

    def halves(v):
        h = v.astype(bf16)
        return h, (v - h.astype(f32)).astype(bf16)

    def dot(a, b):
        return jnp.dot(a, b, preferred_element_type=f32)

    def dot_t(a, b):
        return lax.dot_general(a, b, (((0,), (0,)), ((), ())), preferred_element_type=f32)

    width = 256
    cols = [pl.ds(n * width, width) for n in range(out.shape[1] // width)]

    def solve(q):
        dh, dl = halves(dbuf[q])
        for n in cols:
            if q == 0:
                p = pbuf[0, :, n]
                s = dot(dh, p) + dot(dl, p)
            else:
                w = pbuf[1, :, n].astype(f32) - dot_t(vbuf[...], solved[0, :, n])
                wh, wl = halves(w)
                s = dot(dh, wh) + dot(dl, wh) + dot(dh, wl)
            solved[q, :, n] = s.astype(bf16)

    def product(rows, q, last):
        lq = [lbuf[k, :, rows] for k in range(q, last + 1)]
        for n in cols:
            o = out[rows, n].astype(f32) if q == 0 else acc[rows, n]
            for k in range(q, last + 1):
                o = o - dot_t(lq[k - q], solved[k, :, n])
            if last == 1:
                out[rows, n] = o.astype(bf16)
            else:
                acc[rows, n] = o

    load_l.wait()
    for q in range(2):
        pl.when(is_src[q])(load_p[q].wait)
    act = {"oz": ev_oz, "ou": ev_ou, "od": ev_od, "z": ev_z, "f": ev_f, "g": ev_g, "o": ev_o,
           "zf": ev_zf, "zg": ev_zg, "zo": ev_zo, "done": ev_done}
    chunks = ["V"] + list(range(nchunk))
    skip = False
    for n, step in enumerate(ORDER):
        if n == 15:
            ev_v()
        name, r = step
        if name in act:
            act[name](r)
        elif name == "S":
            if r == 0:
                load_d.wait()
                load_m.wait()
            solve(r)
        elif name == "A":
            skip = ("B", r) == (ORDER + ((),))[n + 1]
            product(rows_of(r), 0, 1 if skip else 0)
        elif name == "B":
            if not skip:
                product(rows_of(r), 1, 1)
            skip = False
        else:
            @pl.when(aux == name)
            def _(a=name, todo=r):
                for what, q, i in todo:
                    pivot(a, what, q, i)

    for r in chunks:
        ev_sent(r)
    for a in sent:
        @pl.when(aux == a)
        def _(a=a):
            for q, i, k, whole in sent[a]:
                ref = pbuf.at[q, pl.ds(i * piece, piece if whole else half), :]
                p_copy(q, i, k, ref, ref, "y+", p_recv.at[q, i]).wait_send()

    @pl.when(is_src[1])
    def _():
        for k in range(1, 8):
            v_copy(k).wait_send()


def finish(part, lbuf, solved, out_hbm, solved_hbm, late, sems):
    f32, bf16 = jnp.float32, jnp.bfloat16
    n_sem = iter(range(2 + 2 * len(CHUNKS)))
    copies = [pltpu.make_async_copy(solved, solved_hbm, sems.at[next(n_sem)])]
    ready = sorted(CHUNKS[r] for r in range(len(CHUNKS)) if r not in TAIL)
    runs = []
    for start, size in ready:
        if runs and runs[-1][0] + runs[-1][1] == start:
            runs[-1][1] += size
        else:
            runs.append([start, size])
    for start, size in runs:
        rows = pl.ds(start, size)
        copies.append(pltpu.make_async_copy(part.at[rows, :], out_hbm.at[rows, :], sems.at[next(n_sem)]))
    for copy in copies:
        copy.start()
    base = 0
    width = 256
    for r in TAIL:
        start, size = CHUNKS[r]
        rows = pl.ds(start, size)
        lq = [lbuf[k, :, rows] for k in range(2)]
        for c in range(part.shape[1] // width):
            n = pl.ds(c * width, width)
            o = part[rows, n].astype(f32)
            for k in range(2):
                o = o - lax.dot_general(lq[k], solved[k, :, n], (((0,), (0,)), ((), ())), preferred_element_type=f32)
            late[pl.ds(base, size), n] = o.astype(bf16)
            if c % 2:
                pair_cols = pl.ds((c - 1) * width, 2 * width)
                copy = pltpu.make_async_copy(late.at[pl.ds(base, size), pair_cols], out_hbm.at[rows, pair_cols], sems.at[next(n_sem)])
                copy.start()
                copies.append(copy)
        base += size
    for copy in copies:
        copy.wait()


def solution(mesh):
    def step(m_panels, lower_cols, diag_inverses):
        rows, cols = m_panels.shape
        panels, nk, _ = diag_inverses.shape
        dma = pltpu.SemaphoreType.DMA
        n = len(TYPES) + 1
        bf16 = jnp.bfloat16
        part, solved, lbuf = pl.pallas_call(
            kernel,
            out_shape=(
                pltpu.VMEM((rows, cols), bf16),
                pltpu.VMEM((panels, nk, cols), bf16),
                pltpu.VMEM((panels, nk, rows), bf16),
            ),
            in_specs=[pl.BlockSpec(memory_space=pltpu.HBM)] * 3,
            out_specs=(pl.BlockSpec(memory_space=pltpu.VMEM),) * 3,
            scratch_shapes=[
                pltpu.VMEM((panels, nk, cols), bf16),
                pltpu.VMEM((panels, nk // 2, cols), bf16),
                pltpu.VMEM((nk, nk), bf16),
                pltpu.VMEM((panels, nk, nk), jnp.float32),
                pltpu.VMEM((rows, cols), jnp.float32),
                dma((5,)), dma((n, 7)), dma((n,)), dma((n,)), dma((1,)), dma((8,)),
                dma((panels, NP)), dma((panels, NP)), dma((panels, NP, 5)), pltpu.SemaphoreType.REGULAR,
            ],
            compiler_params=pltpu.CompilerParams(collective_id=0, has_side_effects=True, vmem_limit_bytes=36 * 2**20),
        )(m_panels, lower_cols, diag_inverses)
        late = -(-sum(CHUNKS[r][1] for r in TAIL) // 16) * 16
        return pl.pallas_call(
            finish,
            out_shape=(jax.ShapeDtypeStruct((rows, cols), bf16), jax.ShapeDtypeStruct((panels, nk, cols), bf16)),
            in_specs=[pl.BlockSpec(memory_space=pltpu.VMEM)] * 3,
            out_specs=(pl.BlockSpec(memory_space=pltpu.HBM),) * 2,
            scratch_shapes=[pltpu.VMEM((late, cols), bf16), dma((2 + 2 * len(CHUNKS),))],
            compiler_params=pltpu.CompilerParams(vmem_limit_bytes=12 * 2**20),
        )(*(pltpu.with_memory_space_constraint(v, pltpu.VMEM) for v in (part, lbuf, solved)))

    return jax.shard_map(
        step,
        mesh=mesh,
        in_specs=(P("aux", "pair"), P(None, "pair", "aux"), P()),
        out_specs=(P("aux", "pair"), P(None, None, "pair")),
        check_vma=False,
    )
```
